32 devices in a mesh: groups: 2 (over x), shard: 16 (over z, y, core).
Axes of the slice: x: 2, y: 2, z: 4, core: 2. Of those that a mesh axis runs over, the one named last changes fastest.
Arguments:
- echoes: float32 [1, 2, 4, 512, 8192], P(None, None, 'groups', 'shard'), parts along dimension 2, may hold values from -6 to 6
- waveform: float32 [2, 8192], replicated, may hold values from -6 to 6
- doppler_taper: float32 [512], replicated, may hold values from 0.3 to 1
- cfar_guard: int32 [4], P('groups'), parts along dimension 0, may hold values from 1 to 4, as said below
- cfar_train: int32 [4], P('groups'), parts along dimension 0, may hold values from 2 to 16
- noise_floor: float32 [4], P('groups'), parts along dimension 0, may hold values from 0.5 to 2
Outputs:
- cfar_ratio: float32 [1, 4, 512, 8192], P(None, 'groups', None, 'shard'), parts along dimension 1
The draws below stay inside these ranges and needn't reach their ends.
There are 2 independent parts, one for each index of `groups`. The reference program is written for one: setup_inputs(seed, part) draws one part's arguments, and reference() takes and returns one part's arrays. A program takes and returns all parts, laid end to end along the dimension named above; an argument that names none is the same for every part. Nothing has to cross between parts.
Inputs may be any that keep to these rules, and one draw needn't show every extreme that they name: In every draw some beam has cfar_guard 4 together with cfar_train 16; no beam has more of either.
All inputs are finite; a program needn't handle non-finite values.
Results may differ from the reference program's by a relative error of at most 0.000075.
Values sent between devices are 32-bit elements; how exact they have to be, the bound alone decides.
A program may use at most 64 MiB of HBM per device.

```python
import math
import jax
import jax.numpy as jnp

NCPI = 1
BEAMS = 2
PULSES = 512
GATES = 8192
GUARD_MAX = 4
TRAIN_MAX = 16
HALO = 20


def cfar_windows(key):
    guard_key = jax.random.fold_in(key, 11)
    train_key = jax.random.fold_in(key, 12)
    pick_key = jax.random.fold_in(key, 13)
    guard_cells = jax.random.randint(guard_key, (BEAMS,), 1, GUARD_MAX + 1)
    train_cells = jax.random.randint(train_key, (BEAMS,), 2, TRAIN_MAX + 1)
    chosen = jax.random.randint(pick_key, (), 0, BEAMS)
    widest = jnp.arange(BEAMS) == chosen
    guard_cells = jnp.where(widest, GUARD_MAX, guard_cells)
    train_cells = jnp.where(widest, TRAIN_MAX, train_cells)
    return (guard_cells.astype(jnp.int32), train_cells.astype(jnp.int32))


def draw_cfar_guard(key, part):
    return cfar_windows(key)[0]


def draw_cfar_train(key, part):
    return cfar_windows(key)[1]


def block_scale(stream_key, dims, pieces, smallest, top_value):
    def one(axis_at, blocks):
        heights = jax.random.uniform(jax.random.fold_in(jax.random.fold_in(stream_key, 6), axis_at), (blocks,), jnp.float32, smallest / len(pieces), top_value / len(pieces))
        return jnp.repeat(jnp.exp(heights), dims[axis_at] // blocks).reshape((-1,) + (1,) * (len(dims) - axis_at - 1))

    level = one(*pieces[0])
    for cut in pieces[1:]:
        level = level * one(*cut)
    return level


def normal_values(stream_key, dims, width, reach, cuts=(), kind=jnp.bfloat16):
    level = block_scale(stream_key, dims, cuts, -0.22, 0.18) if cuts else 1.0
    result = jax.random.normal(stream_key, dims, jnp.float32) * width * level
    return jnp.minimum(jnp.maximum(result, -reach), reach).astype(kind)


def setup_inputs(seed: int = 0, part: int = 0) -> dict:
    key_list = jax.random.split(jax.random.key(seed), 7)
    part_keys = jax.random.split(jax.random.fold_in(key_list[6], part), 7)
    echoes = normal_values(part_keys[0], (NCPI, 2, BEAMS, PULSES, GATES), 1.0, 6.0, ((3, 16),), jnp.float32)
    waveform = normal_values(key_list[1], (2, GATES), 1.0, 6.0, (), jnp.float32)
    doppler_taper = jnp.clip(jnp.exp(jax.random.uniform(key_list[2], (PULSES,), jnp.float32, math.log(0.3), math.log(1.0))), 0.3, 1.0)
    cfar_guard = draw_cfar_guard(jax.random.fold_in(jax.random.fold_in(key_list[6], part), 71), part)
    cfar_train = draw_cfar_train(jax.random.fold_in(jax.random.fold_in(key_list[6], part), 71), part)
    noise_floor = jnp.clip(jnp.exp(jax.random.uniform(part_keys[5], (BEAMS,), jnp.float32, math.log(0.5), math.log(2.0))), 0.5, 2.0)
    return dict(echoes=echoes, waveform=waveform, doppler_taper=doppler_taper, cfar_guard=cfar_guard, cfar_train=cfar_train, noise_floor=noise_floor)


def reference(echoes, waveform, doppler_taper, cfar_guard, cfar_train, noise_floor):
    signal = echoes[:, 0] + 1j * echoes[:, 1]
    spectrum = jnp.fft.fft(signal, axis=-1)
    matched = waveform[0] - 1j * waveform[1]
    compressed = jnp.fft.ifft(spectrum * matched, axis=-1)
    tapered = compressed * doppler_taper[:, None]
    doppler = jnp.fft.fft(tapered, axis=2) / jnp.sqrt(jnp.float32(PULSES))
    power_map = jnp.real(doppler) ** 2 + jnp.imag(doppler) ** 2
    padded = jnp.pad(power_map, ((0, 0), (0, 0), (0, 0), (HALO, HALO)))
    offsets = jnp.arange(1, HALO + 1, dtype=jnp.int32)
    inside = (offsets[None, :] > cfar_guard[:, None]) & (offsets[None, :] <= (cfar_guard + cfar_train)[:, None])
    weights = inside.astype(jnp.float32)
    window_sum = jnp.zeros_like(power_map)
    for offset in range(1, HALO + 1):
        lower = padded[..., HALO - offset:HALO - offset + GATES]
        upper = padded[..., HALO + offset:HALO + offset + GATES]
        window_sum = window_sum + weights[:, offset - 1][None, :, None, None] * (lower + upper)
    noise_mean = window_sum / (2.0 * cfar_train.astype(jnp.float32))[None, :, None, None]
    return power_map / (noise_floor[None, :, None, None] + noise_mean)
```

```python
import functools
import math

import jax
import jax.numpy as jnp
import numpy as np
from jax import lax
from jax.experimental import pallas as pl
from jax.experimental.pallas import tpu as pltpu
from jax.sharding import PartitionSpec as P

GB = 128
ROWS = 8
EDGE = 24
MESH = pl.DeviceIdType.MESH


def split(table):
    table = np.asarray(table, np.float32)
    high = table.astype(jnp.bfloat16)
    low = (table - high.astype(np.float32)).astype(jnp.bfloat16)
    return high, low


def dft(length, size=None):
    size = size or length
    i = np.arange(size)[:, None] * np.arange(length)[None, :] % length
    angles = 2.0 * np.pi / length * i
    return np.cos(angles), np.sin(angles)


def tables(gates, pulses):
    ga = gates // GB
    ca, sa = dft(ga)
    cb, sb = dft(GB)

    def left(matrix):
        high, low = split(matrix)
        return np.block([[high, high], [low, np.zeros_like(low)]])

    first = left(np.block([[ca, sa], [-sa, ca]]))
    last = left(np.block([[ca, -sa], [sa, ca]]))
    per = GB // ga
    c = np.arange(GB).reshape(GB // per, per).T.reshape(-1)
    cb, sb = cb[:, c], sb[:, c]
    second = np.stack(split(np.block([[cb, -sb], [sb, cb]])))
    third = np.stack(split(np.block([[cb.T, sb.T], [-sb.T, cb.T]])))
    i = np.arange(ga)[:, None] * np.arange(GB)[None, :] % gates
    twiddle = np.stack([np.cos(2 * np.pi / gates * i), np.sin(2 * np.pi / gates * i)])
    half = pulses // 2
    cp, sp = dft(pulses)
    doppler = [
        np.stack(split(np.concatenate([cp[e::2, :half], sp[e::2, :half]], axis=0))) for e in range(2)
    ]
    return first, second, third, last, twiddle.astype(np.float32), np.stack(doppler)


def parts(x):
    high = x.astype(jnp.bfloat16)
    low = (x - high.astype(jnp.float32)).astype(jnp.bfloat16)
    return high, low


def dot(a, b):
    return jnp.dot(a, b, preferred_element_type=jnp.float32)


def kernel(
    n, beams, pulses, gates,
    echoes, waveform_hbm, taper_hbm, guard_hbm, train_hbm, floor_hbm,
    first_hbm, second_hbm, third_hbm, last_hbm, twiddle_hbm, doppler_hbm,
    out,
    xin, xs, wave, filt, sent, got, table, rhs, power, own, cross, edge, halo, band,
    waveform, taper, guard, train, floor, first, second, third, last, twiddle,
    in_sem, small_sem, table_sem, send_sem, recv_sem, edge_send, edge_recv,
):
    me = lax.axis_index("shard")
    ga = gates // GB
    tiles = ga // n
    groups = pulses // n // ROWS
    half = pulses // 2
    order = sorted(range(1, n), key=lambda k: (abs(2 * k - n), k))

    barrier = pltpu.get_barrier_semaphore()
    for k in order:
        pl.semaphore_signal(
            barrier, inc=1, device_id={"shard": lax.rem(me + k, n)}, device_id_type=MESH
        )

    def load(b, pg):
        start = pg * ROWS if isinstance(pg, int) else pl.multiple_of(pg * ROWS, ROWS)
        return pltpu.make_async_copy(
            echoes.at[0, :, b, pl.ds(start, ROWS), :], xin.at[b, pg], in_sem.at[b, pg]
        )

    small = [
        pltpu.make_async_copy(src, dst, small_sem.at[i])
        for i, (src, dst) in enumerate(
            (
                (waveform_hbm, waveform), (taper_hbm, taper), (first_hbm, first),
                (twiddle_hbm, twiddle), (second_hbm, second), (third_hbm, third), (last_hbm, last),
                (guard_hbm, guard), (train_hbm, train), (floor_hbm, floor),
            )
        )
    ]
    table_copy = pltpu.make_async_copy(doppler_hbm, table, table_sem)
    small[0].start()
    load(0, 0).start()
    for copy in small[1:]:
        copy.start()
    for b in range(beams):
        for pg in range(groups):
            if b or pg:
                load(b, pg).start()
    table_copy.start()

    per = GB // ga
    scale = 1.0 / (gates * math.sqrt(pulses))
    small[0].wait()
    for c in range(2):
        for m in range(ga):
            wave[m:m + 1, :] = waveform[c:c + 1, m * GB:(m + 1) * GB]
        lines = wave[...] * scale
        turned = [lines] + [pltpu.roll(lines, GB - h * ga, axis=1) for h in range(1, per)]
        filt[c] = jnp.concatenate(turned, axis=0).T[:ga]
    for copy in small[1:]:
        copy.wait()

    def stacked(ref):
        return jnp.concatenate([ref[0], ref[0], ref[1]], axis=0)

    def compress(b, pg):
        load(b, pg).wait()
        for c in range(2):
            for i in range(ga):
                xs[c, i * ROWS:(i + 1) * ROWS, :] = xin[b, pg, c, :, i * GB:(i + 1) * GB]
        tc, ts = twiddle[0], twiddle[1]
        lhs = []
        for p in range(0, ROWS, 2):
            x = jnp.concatenate(
                [
                    jnp.concatenate([xs[c, pl.ds(p + e, ga, stride=ROWS), :] for c in range(2)], axis=0)
                    for e in range(2)
                ],
                axis=1,
            )
            y = dot(first[...], jnp.concatenate(parts(x), axis=0))
            y = y[:2 * ga] + y[2 * ga:]
            for e in range(2):
                yr, yi = y[:ga, e * GB:(e + 1) * GB], y[ga:, e * GB:(e + 1) * GB]
                z = jnp.concatenate([yr * tc + yi * ts, yi * tc - yr * ts], axis=1)
                high, low = parts(z)
                lhs.append(jnp.concatenate([high, low, high], axis=1))
        x = dot(jnp.concatenate(lhs, axis=0), stacked(second))
        lhs = []
        fr, fi = filt[0], filt[1]
        for p in range(ROWS):
            weight = taper[(me * groups + pg) * ROWS + p]
            hr, hi = fr * weight, fi * weight
            xr, xi = x[p * ga:(p + 1) * ga, :GB], x[p * ga:(p + 1) * ga, GB:]
            z = jnp.concatenate([xr * hr + xi * hi, xi * hr - xr * hi], axis=1)
            high, low = parts(z)
            lhs.append(jnp.concatenate([high, low, high], axis=1))
        x = dot(jnp.concatenate(lhs, axis=0), stacked(third))
        for p in range(0, ROWS, 2):
            pair = []
            for e in range(2):
                r = (p + e) * ga
                xr, xi = x[r:r + ga, :GB], x[r:r + ga, GB:]
                pair.append(jnp.concatenate([xr * tc - xi * ts, xi * tc + xr * ts], axis=0))
            y = dot(last[...], jnp.concatenate(parts(jnp.concatenate(pair, axis=1)), axis=0))
            y = y[:2 * ga] + y[2 * ga:]
            for e in range(2):
                for c in range(2):
                    sent.at[b, c, pg].reshape(ga * ROWS, GB)[pl.ds(p + e, ga, stride=ROWS), :] = y[
                        c * ga:(c + 1) * ga, e * GB:(e + 1) * GB
                    ]

    def send_group(b, pg):
        dst = got.at[b, :, :, me * groups + pg]
        for k in order:
            to = lax.rem(me + k, n)
            pltpu.make_async_remote_copy(
                src_ref=sent.at[b, :, pg, pl.ds(to * tiles, tiles)],
                dst_ref=dst,
                send_sem=send_sem.at[b],
                recv_sem=recv_sem.at[b, 0],
                device_id={"shard": to},
                device_id_type=MESH,
            ).start()
        pltpu.make_async_copy(
            sent.at[b, :, pg, pl.ds(me * tiles, tiles)], dst, recv_sem.at[b, 0]
        ).start()

    def send_tile(b, j):
        dst = got.at[b, :, j, pl.ds(me * groups, groups)]
        for k in order:
            to = lax.rem(me + k, n)
            pltpu.make_async_remote_copy(
                src_ref=sent.at[b, :, :, to * tiles + j],
                dst_ref=dst,
                send_sem=send_sem.at[b],
                recv_sem=recv_sem.at[b, j],
                device_id={"shard": to},
                device_id_type=MESH,
            ).start()
        pltpu.make_async_copy(sent.at[b, :, :, me * tiles + j], dst, recv_sem.at[b, j]).start()

    for b in range(beams):
        final = b == beams - 1

        @pl.loop(0, groups)
        def _(pg):
            compress(b, pg)
            if b == 0:
                @pl.when(pg == 0)
                def _():
                    pl.semaphore_wait(barrier, n - 1)

            if not final:
                send_group(b, pg)

        if final:
            @pl.loop(0, tiles)
            def _(t):
                send_tile(b, lax.rem(t * (tiles - 1), tiles))

    table_copy.wait()

    m = lax.broadcasted_iota(jnp.int32, (GB, 2 * GB), 0)
    k = lax.broadcasted_iota(jnp.int32, (GB, 2 * GB), 1)
    apart = jnp.where(k < GB, jnp.abs(m - k), jnp.where(k < GB + GB // 2, k - m, m + 2 * GB - k))
    for b in range(beams):
        inside = (apart > guard[b]) & (apart <= guard[b] + train[b])
        lines = jnp.where(inside, 1.0, 0.0).astype(jnp.bfloat16)
        band[b, :GB] = lines
        band[b, GB:] = lines

    def sums(b, x):
        return dot(jnp.concatenate(parts(x), axis=1), band[b])

    def transform(b, j, then=None):
        x = jnp.concatenate([got[b, c, j].reshape(pulses, GB) for c in range(2)], axis=1)
        for e, y in enumerate((x[:half] + x[half:], x[:half] - x[half:])):
            high, low = parts(y)
            rhs[e, 0:half] = high
            rhs[e, half:2 * half] = low
            rhs[e, 2 * half:] = high
        for e in range(2):
            lhs = jnp.concatenate([table[e, 0], table[e, 0], table[e, 1]], axis=1)
            spec = dot(lhs, rhs[e])
            re = spec[:half, :GB] + spec[half:, GB:]
            im = spec[:half, GB:] - spec[half:, :GB]
            p = re * re + im * im
            power[b, j, e] = p
            total = sums(b, p)
            own[b, j, e] = total[:, :GB]
            cross[b, j + 1, e] = total[:, GB:]
            if then is not None:
                then(e)

    def ratio(b, j, e):
        lower = lax.broadcasted_iota(jnp.int32, (half, GB), 1) < GB // 2
        twice = 2.0 * train[b].astype(jnp.float32)
        base = floor[b] * twice
        total = own[b, j, e] + jnp.where(lower, cross[b, j, e], cross[b, j + 2, e])
        out.at[b, j][pl.ds(e, half, stride=2), :] = power[b, j, e] * twice / (base + total)

    def edge_copy(b, side):
        to = lax.rem(me + (n - 1 if side == 0 else 1), n)
        return pltpu.make_async_remote_copy(
            src_ref=edge.at[b, side],
            dst_ref=halo.at[b, side],
            send_sem=edge_send.at[b, side],
            recv_sem=edge_recv.at[b, side],
            device_id={"shard": to},
            device_id_type=MESH,
        )

    def send_edges(b):
        for e in range(2):
            rows = slice(e * half, (e + 1) * half)
            edge[b, 0, :, rows] = power[b, 0, e].T[:EDGE]
            edge[b, 1, :, rows] = power[b, tiles - 1, e].T[GB - EDGE:]
        for side in range(2):
            edge_copy(b, side).start()

    def take_edges(b):
        for side in range(2):
            edge_copy(b, side).wait()
        after = jnp.where(me < n - 1, halo[b, 0], 0.0)
        before = jnp.where(me > 0, halo[b, 1], 0.0)
        zeros = jnp.zeros((GB - 2 * EDGE, half), jnp.float32)
        for e in range(2):
            rows = slice(e * half, (e + 1) * half)
            x = jnp.concatenate([after[:, rows], zeros, before[:, rows]], axis=0).T
            total = sums(b, x)[:, GB:]
            cross[b, 0, e] = total
            cross[b, tiles + 1, e] = total

    for b in range(beams - 1):
        pltpu.make_async_copy(got.at[b], got.at[b], recv_sem.at[b, 0]).wait()

        @pl.loop(0, tiles)
        def _(j):
            transform(b, j)

        send_edges(b)

    b = beams - 1
    done = set()
    ready = set()

    def ratios(e):
        for j in range(tiles):
            if j not in done and {j - 1, j, j + 1} & set(range(tiles)) <= ready:
                ratio(b, j, e)
                if e == 1:
                    done.add(j)

    for t in range(tiles):
        j = t * (tiles - 1) % tiles
        arrived = got.at[b, :, j]
        pltpu.make_async_copy(arrived, arrived, recv_sem.at[b, j]).wait()
        ready.add(j)
        transform(b, j, ratios if 2 < tiles == t + 1 else None)
        if t == min(1, tiles - 1):
            send_edges(b)
        if t == max(tiles - 2, min(1, tiles - 1)):
            for i in range(beams):
                take_edges(i)
            for i in range(beams - 1):
                for jj in range(tiles):
                    for e in range(2):
                        ratio(i, jj, e)
            for e in range(2):
                ratios(e)

    for b in range(beams):
        whole = sent.at[b, :, :, pl.ds(0, (n - 1) * tiles)]
        pltpu.make_async_copy(whole, whole, send_sem.at[b]).wait()


def write_kernel(ratio, out, sem):
    beams, tiles = ratio.shape[:2]
    copies = [
        pltpu.make_async_copy(ratio.at[b, j], out.at[0, b, :, pl.ds(j * GB, GB)], sem.at[b, j])
        for b in range(beams)
        for j in range(tiles)
    ]
    for copy in copies:
        copy.start()
    for copy in copies:
        copy.wait()


def solution(mesh):
    n = mesh.shape["shard"]

    def step(echoes, waveform, doppler_taper, cfar_guard, cfar_train, noise_floor):
        beams, local, gates = echoes.shape[2:]
        pulses = local * n
        ga = gates // GB
        tiles = ga // n
        groups = local // ROWS
        half = pulses // 2
        consts = tables(gates, pulses)
        first, second, third, last, twiddle, doppler = consts
        vmem = pl.BlockSpec(memory_space=pltpu.VMEM)
        hbm = pl.BlockSpec(memory_space=pltpu.HBM)
        f32, bf16, i32 = jnp.float32, jnp.bfloat16, jnp.int32
        dma = pltpu.SemaphoreType.DMA
        room = 65472 * 1024 - 4 * beams * tiles * pulses * GB - 16 * 1024
        ratio = pl.pallas_call(
            functools.partial(kernel, n, beams, pulses, gates),
            out_shape=pltpu.VMEM((beams, tiles, pulses, GB), f32),
            in_specs=[hbm] * 12,
            out_specs=vmem,
            scratch_shapes=[
                pltpu.VMEM((beams, groups, 2, ROWS, gates), f32),
                pltpu.VMEM((2, ga * ROWS, GB), f32),
                pltpu.VMEM((ga, GB), f32),
                pltpu.VMEM((2, ga, GB), f32),
                pltpu.VMEM((beams, 2, groups, ga, ROWS, GB), f32),
                pltpu.VMEM((beams, 2, tiles, pulses // ROWS, ROWS, GB), f32),
                pltpu.VMEM((2, 2, pulses, half), bf16),
                pltpu.VMEM((2, 3 * half, 2 * GB), bf16),
                pltpu.VMEM((beams, tiles, 2, half, GB), f32),
                pltpu.VMEM((beams, tiles, 2, half, GB), f32),
                pltpu.VMEM((beams, tiles + 2, 2, half, GB), f32),
                pltpu.VMEM((beams, 2, EDGE, pulses), f32),
                pltpu.VMEM((beams, 2, EDGE, pulses), f32),
                pltpu.VMEM((beams, 2 * GB, 2 * GB), bf16),
                pltpu.VMEM((2, gates), f32),
                pltpu.SMEM((pulses,), f32),
                pltpu.SMEM((beams,), i32),
                pltpu.SMEM((beams,), i32),
                pltpu.SMEM((beams,), f32),
                pltpu.VMEM(first.shape, bf16),
                pltpu.VMEM(second.shape, bf16),
                pltpu.VMEM(third.shape, bf16),
                pltpu.VMEM(last.shape, bf16),
                pltpu.VMEM(twiddle.shape, f32),
                dma((beams, groups)),
                dma((10,)),
                dma,
                dma((beams,)),
                dma((beams, tiles)),
                dma((beams, 2)),
                dma((beams, 2)),
            ],
            compiler_params=pltpu.CompilerParams(
                collective_id=0, has_side_effects=True, vmem_limit_bytes=room
            ),
        )(
            echoes, waveform, doppler_taper, cfar_guard, cfar_train, noise_floor,
            *(jnp.asarray(c) for c in consts),
        )
        return pl.pallas_call(
            write_kernel,
            out_shape=jax.ShapeDtypeStruct((1, beams, pulses, tiles * GB), f32),
            in_specs=[vmem],
            out_specs=hbm,
            scratch_shapes=[dma((beams, tiles))],
            compiler_params=pltpu.CompilerParams(vmem_limit_bytes=1024 * 1024),
        )(ratio)

    in_specs = (
        P(None, None, "groups", "shard", None),
        P(),
        P(),
        P("groups"),
        P("groups"),
        P("groups"),
    )
    return jax.shard_map(
        step, mesh=mesh, in_specs=in_specs, out_specs=P(None, "groups", None, "shard"), check_vma=False
    )
```

```python
import functools
import math

import jax
import jax.numpy as jnp
import numpy as np
from jax import lax
from jax.experimental import pallas as pl
from jax.experimental.pallas import tpu as pltpu
from jax.sharding import PartitionSpec as P

GB = 128
ROWS = 8
EDGE = 24
MESH = pl.DeviceIdType.MESH


def split(table):
    table = np.asarray(table, np.float32)
    high = table.astype(jnp.bfloat16)
    low = (table - high.astype(np.float32)).astype(jnp.bfloat16)
    return high, low


def dft(length, size=None):
    size = size or length
    i = np.arange(size)[:, None] * np.arange(length)[None, :] % length
    angles = 2.0 * np.pi / length * i
    return np.cos(angles), np.sin(angles)


def slots(tiles):
    return [0, tiles - 1, *range(tiles - 2, 0, -1)][:tiles]


def tables(gates, pulses, n):
    ga = gates // GB
    tiles = ga // n
    rows = (np.arange(0, ga, tiles)[:, None] + np.array(slots(tiles))[None, :]).reshape(-1)
    ca, sa = dft(ga)
    cb, sb = dft(GB)

    def left(matrix):
        high, low = split(matrix)
        return np.block([[high, high], [low, np.zeros_like(low)]])

    first = left(np.block([[ca, sa], [-sa, ca]]))
    last = left(np.block([[ca[rows], -sa[rows]], [sa[rows], ca[rows]]]))
    per = GB // ga
    c = np.arange(GB).reshape(GB // per, per).T.reshape(-1)
    cb, sb = cb[:, c], sb[:, c]
    second = np.stack(split(np.block([[cb, -sb], [sb, cb]])))
    third = np.stack(split(np.block([[cb.T, sb.T], [-sb.T, cb.T]])))
    i = np.arange(ga)[:, None] * np.arange(GB)[None, :] % gates
    twiddle = np.stack([np.cos(2 * np.pi / gates * i), np.sin(2 * np.pi / gates * i)])
    half = pulses // 2
    cp, sp = dft(pulses)
    doppler = [
        np.stack(split(np.concatenate([cp[e::2, :half], sp[e::2, :half]], axis=0))) for e in range(2)
    ]
    return first, second, third, last, twiddle.astype(np.float32), np.stack(doppler)


def parts(x):
    high = x.astype(jnp.bfloat16)
    low = (x - high.astype(jnp.float32)).astype(jnp.bfloat16)
    return high, low


def dot(a, b):
    return jnp.dot(a, b, preferred_element_type=jnp.float32)


def kernel(
    n, beams, pulses, gates,
    echoes, waveform_hbm, taper_hbm, guard_hbm, train_hbm, floor_hbm,
    first_hbm, second_hbm, third_hbm, last_hbm, twiddle_hbm, doppler_hbm,
    out,
    xin, xs, wave, filt, sent, got, table, rhs, power, own, cross, edge, halo, band,
    waveform, taper, guard, train, floor, first, second, third, last, twiddle,
    in_sem, small_sem, table_sem, send_sem, recv_sem, edge_send, edge_recv,
):
    me = lax.axis_index("shard")
    ga = gates // GB
    tiles = ga // n
    groups = pulses // n // ROWS
    half = pulses // 2
    place = slots(tiles)
    outer = min(2, tiles)
    side = n // 2
    mine = lax.rem(me, side)
    far, here = side - (me - mine), me - mine
    across = [far + k for k in range(side)]
    near = [here + lax.rem(mine + k, side) for k in range(1, side)]
    order = across[:1] + [to for pair in zip(near, across[1:]) for to in pair]

    barrier = pltpu.get_barrier_semaphore()
    for to in order:
        pl.semaphore_signal(barrier, inc=1, device_id={"shard": to}, device_id_type=MESH)

    def load(b, pg):
        start = pg * ROWS if isinstance(pg, int) else pl.multiple_of(pg * ROWS, ROWS)
        return pltpu.make_async_copy(
            echoes.at[0, :, b, pl.ds(start, ROWS), :], xin.at[b, pg], in_sem.at[b, pg]
        )

    small = [
        pltpu.make_async_copy(src, dst, small_sem.at[i])
        for i, (src, dst) in enumerate(
            (
                (waveform_hbm, waveform), (taper_hbm, taper), (first_hbm, first),
                (twiddle_hbm, twiddle), (second_hbm, second), (third_hbm, third), (last_hbm, last),
                (guard_hbm, guard), (train_hbm, train), (floor_hbm, floor),
            )
        )
    ]
    table_copy = pltpu.make_async_copy(doppler_hbm, table, table_sem)
    small[0].start()
    load(0, 0).start()
    for copy in small[1:]:
        copy.start()

    per = GB // ga
    scale = 1.0 / (gates * math.sqrt(pulses))
    small[0].wait()
    for c in range(2):
        for m in range(ga):
            wave[m:m + 1, :] = waveform[c:c + 1, m * GB:(m + 1) * GB]
        lines = wave[...] * scale
        turned = [lines] + [pltpu.roll(lines, GB - h * ga, axis=1) for h in range(1, per)]
        filt[c] = jnp.concatenate(turned, axis=0).T[:ga]
    for copy in small[1:]:
        copy.wait()
    load(0, 0).wait()
    for b in range(beams):
        for pg in range(groups):
            if b or pg:
                load(b, pg).start()
    table_copy.start()

    def stacked(ref):
        return jnp.concatenate([ref[0], ref[0], ref[1]], axis=0)

    def compress(b, pg):
        if b:
            load(b, pg).wait()
        else:
            @pl.when(pg > 0)
            def _():
                load(b, pg).wait()

        for c in range(2):
            for i in range(ga):
                xs[c, i * ROWS:(i + 1) * ROWS, :] = xin[b, pg, c, :, i * GB:(i + 1) * GB]
        tc, ts = twiddle[0], twiddle[1]
        lhs = []
        for p in range(0, ROWS, 2):
            x = jnp.concatenate(
                [
                    jnp.concatenate([xs[c, pl.ds(p + e, ga, stride=ROWS), :] for c in range(2)], axis=0)
                    for e in range(2)
                ],
                axis=1,
            )
            y = dot(first[...], jnp.concatenate(parts(x), axis=0))
            y = y[:2 * ga] + y[2 * ga:]
            for e in range(2):
                yr, yi = y[:ga, e * GB:(e + 1) * GB], y[ga:, e * GB:(e + 1) * GB]
                z = jnp.concatenate([yr * tc + yi * ts, yi * tc - yr * ts], axis=1)
                high, low = parts(z)
                lhs.append(jnp.concatenate([high, low, high], axis=1))
        x = dot(jnp.concatenate(lhs, axis=0), stacked(second))
        lhs = []
        fr, fi = filt[0], filt[1]
        for p in range(ROWS):
            weight = taper[(me * groups + pg) * ROWS + p]
            hr, hi = fr * weight, fi * weight
            xr, xi = x[p * ga:(p + 1) * ga, :GB], x[p * ga:(p + 1) * ga, GB:]
            z = jnp.concatenate([xr * hr + xi * hi, xi * hr - xr * hi], axis=1)
            high, low = parts(z)
            lhs.append(jnp.concatenate([high, low, high], axis=1))
        x = dot(jnp.concatenate(lhs, axis=0), stacked(third))
        for p in range(0, ROWS, 2):
            pair = []
            for e in range(2):
                r = (p + e) * ga
                xr, xi = x[r:r + ga, :GB], x[r:r + ga, GB:]
                pair.append(jnp.concatenate([xr * tc - xi * ts, xi * tc + xr * ts], axis=0))
            y = dot(last[...], jnp.concatenate(parts(jnp.concatenate(pair, axis=1)), axis=0))
            y = y[:2 * ga] + y[2 * ga:]
            for e in range(2):
                for c in range(2):
                    sent.at[b, c, pg].reshape(ga * ROWS, GB)[pl.ds(p + e, ga, stride=ROWS), :] = y[
                        c * ga:(c + 1) * ga, e * GB:(e + 1) * GB
                    ]

    def send(src, dst, b, sem, peers, keep):
        for to in peers:
            pltpu.make_async_remote_copy(
                src_ref=src(to),
                dst_ref=dst,
                send_sem=send_sem.at[b],
                recv_sem=recv_sem.at[b, sem],
                device_id={"shard": to},
                device_id_type=MESH,
            ).start()
        if keep:
            pltpu.make_async_copy(src(me), dst, recv_sem.at[b, sem]).start()

    def send_group(b, pg):
        send(
            lambda to: sent.at[b, :, pg, pl.ds(to * tiles, outer)],
            got.at[b, :, pl.ds(0, outer), me * groups + pg],
            b, 0, order, True,
        )

    def send_slot(b, t, peers, keep):
        send(
            lambda to: sent.at[b, :, :, to * tiles + t],
            got.at[b, :, t, pl.ds(me * groups, groups)],
            b, t, peers, keep,
        )

    for b in range(beams):

        @pl.loop(0, groups)
        def _(pg):
            compress(b, pg)
            if b == 0:
                @pl.when(pg == 0)
                def _():
                    pl.semaphore_wait(barrier, n - 1)

            send_group(b, pg)

    for t in range(outer, tiles - 1):
        for b in range(beams):
            send_slot(b, t, order, True)

    table_copy.wait()

    m = lax.broadcasted_iota(jnp.int32, (GB, 2 * GB), 0)
    k = lax.broadcasted_iota(jnp.int32, (GB, 2 * GB), 1)
    apart = jnp.where(k < GB, jnp.abs(m - k), jnp.where(k < GB + GB // 2, k - m, m + 2 * GB - k))
    for b in range(beams):
        inside = (apart > guard[b]) & (apart <= guard[b] + train[b])
        lines = jnp.where(inside, 1.0, 0.0).astype(jnp.bfloat16)
        band[b, :GB] = lines
        band[b, GB:] = lines

    def sums(b, x):
        return dot(jnp.concatenate(parts(x), axis=1), band[b])

    def transform(b, t, then=None):
        j = place[t]
        x = jnp.concatenate([got[b, c, t].reshape(pulses, GB) for c in range(2)], axis=1)
        for e, y in enumerate((x[:half] + x[half:], x[:half] - x[half:])):
            high, low = parts(y)
            rhs[e, 0:half] = high
            rhs[e, half:2 * half] = low
            rhs[e, 2 * half:] = high
        for e in range(2):
            lhs = jnp.concatenate([table[e, 0], table[e, 0], table[e, 1]], axis=1)
            spec = dot(lhs, rhs[e])
            re = spec[:half, :GB] + spec[half:, GB:]
            im = spec[:half, GB:] - spec[half:, :GB]
            p = re * re + im * im
            power[b, j, e] = p
            total = sums(b, p)
            own[b, j, e] = total[:, :GB]
            cross[b, j + 1, e] = total[:, GB:]
            if then is not None:
                then(e)

    def ratio(b, j, e):
        lower = lax.broadcasted_iota(jnp.int32, (half, GB), 1) < GB // 2
        twice = 2.0 * train[b].astype(jnp.float32)
        base = floor[b] * twice
        total = own[b, j, e] + jnp.where(lower, cross[b, j, e], cross[b, j + 2, e])
        out.at[b, j][pl.ds(e, half, stride=2), :] = power[b, j, e] * twice / (base + total)

    def edge_copy(b, side):
        to = lax.rem(me + (n - 1 if side == 0 else 1), n)
        return pltpu.make_async_remote_copy(
            src_ref=edge.at[b, side],
            dst_ref=halo.at[b, side],
            send_sem=edge_send.at[b, side],
            recv_sem=edge_recv.at[b, side],
            device_id={"shard": to},
            device_id_type=MESH,
        )

    def send_edges(b):
        for e in range(2):
            rows = slice(e * half, (e + 1) * half)
            edge[b, 0, :, rows] = power[b, 0, e].T[:EDGE]
            edge[b, 1, :, rows] = power[b, tiles - 1, e].T[GB - EDGE:]
        for side in range(2):
            edge_copy(b, side).start()

    def take_edges(b):
        for side in range(2):
            edge_copy(b, side).wait()
        after = jnp.where(me < n - 1, halo[b, 0], 0.0)
        before = jnp.where(me > 0, halo[b, 1], 0.0)
        zeros = jnp.zeros((GB - 2 * EDGE, half), jnp.float32)
        for e in range(2):
            rows = slice(e * half, (e + 1) * half)
            x = jnp.concatenate([after[:, rows], zeros, before[:, rows]], axis=0).T
            total = sums(b, x)[:, GB:]
            cross[b, 0, e] = total
            cross[b, tiles + 1, e] = total

    for b in range(beams):
        arrived = got.at[b, :, pl.ds(0, outer)]
        pltpu.make_async_copy(arrived, arrived, recv_sem.at[b, 0]).wait()
        for t in range(outer):
            transform(b, t)
        send_edges(b)

    if tiles > outer:
        for b in range(beams):
            send_slot(b, tiles - 1, near, True)
        for b in range(beams):
            send_slot(b, tiles - 1, across, False)

    done = [set() for _ in range(beams)]

    def ratios(b, ready, e):
        for j in range(tiles):
            if j not in done[b] and {j - 1, j, j + 1} & set(range(tiles)) <= ready:
                ratio(b, j, e)
                if e == 1:
                    done[b].add(j)

    for t in range(outer, tiles):
        ready = set(place[:t + 1])
        for b in range(beams):
            arrived = got.at[b, :, t]
            pltpu.make_async_copy(arrived, arrived, recv_sem.at[b, t]).wait()
            final = t == tiles - 1
            transform(b, t, functools.partial(ratios, b, ready) if final and t > outer else None)
        if t == max(outer, tiles - 2):
            for b in range(beams):
                take_edges(b)
        if not final or t == outer:
            for b in range(beams):
                for e in range(2):
                    ratios(b, ready, e)
    if tiles == outer:
        for b in range(beams):
            take_edges(b)
            for e in range(2):
                ratios(b, set(range(tiles)), e)

    for b in range(beams):
        whole = sent.at[b, :, :, pl.ds(0, (n - 1) * tiles)]
        pltpu.make_async_copy(whole, whole, send_sem.at[b]).wait()


def write_kernel(ratio, out, sem):
    beams, tiles = ratio.shape[:2]
    copies = [
        pltpu.make_async_copy(ratio.at[b, j], out.at[0, b, :, pl.ds(j * GB, GB)], sem.at[b, j])
        for b in range(beams)
        for j in range(tiles)
    ]
    for copy in copies:
        copy.start()
    for copy in copies:
        copy.wait()


def solution(mesh):
    n = mesh.shape["shard"]

    def step(echoes, waveform, doppler_taper, cfar_guard, cfar_train, noise_floor):
        beams, local, gates = echoes.shape[2:]
        pulses = local * n
        ga = gates // GB
        tiles = ga // n
        groups = local // ROWS
        half = pulses // 2
        consts = tables(gates, pulses, n)
        first, second, third, last, twiddle, doppler = consts
        vmem = pl.BlockSpec(memory_space=pltpu.VMEM)
        hbm = pl.BlockSpec(memory_space=pltpu.HBM)
        f32, bf16, i32 = jnp.float32, jnp.bfloat16, jnp.int32
        dma = pltpu.SemaphoreType.DMA
        room = 65472 * 1024 - 4 * beams * tiles * pulses * GB - 16 * 1024
        ratio = pl.pallas_call(
            functools.partial(kernel, n, beams, pulses, gates),
            out_shape=pltpu.VMEM((beams, tiles, pulses, GB), f32),
            in_specs=[hbm] * 12,
            out_specs=vmem,
            scratch_shapes=[
                pltpu.VMEM((beams, groups, 2, ROWS, gates), f32),
                pltpu.VMEM((2, ga * ROWS, GB), f32),
                pltpu.VMEM((ga, GB), f32),
                pltpu.VMEM((2, ga, GB), f32),
                pltpu.VMEM((beams, 2, groups, ga, ROWS, GB), f32),
                pltpu.VMEM((beams, 2, tiles, pulses // ROWS, ROWS, GB), f32),
                pltpu.VMEM((2, 2, pulses, half), bf16),
                pltpu.VMEM((2, 3 * half, 2 * GB), bf16),
                pltpu.VMEM((beams, tiles, 2, half, GB), f32),
                pltpu.VMEM((beams, tiles, 2, half, GB), f32),
                pltpu.VMEM((beams, tiles + 2, 2, half, GB), f32),
                pltpu.VMEM((beams, 2, EDGE, pulses), f32),
                pltpu.VMEM((beams, 2, EDGE, pulses), f32),
                pltpu.VMEM((beams, 2 * GB, 2 * GB), bf16),
                pltpu.VMEM((2, gates), f32),
                pltpu.SMEM((pulses,), f32),
                pltpu.SMEM((beams,), i32),
                pltpu.SMEM((beams,), i32),
                pltpu.SMEM((beams,), f32),
                pltpu.VMEM(first.shape, bf16),
                pltpu.VMEM(second.shape, bf16),
                pltpu.VMEM(third.shape, bf16),
                pltpu.VMEM(last.shape, bf16),
                pltpu.VMEM(twiddle.shape, f32),
                dma((beams, groups)),
                dma((10,)),
                dma,
                dma((beams,)),
                dma((beams, tiles)),
                dma((beams, 2)),
                dma((beams, 2)),
            ],
            compiler_params=pltpu.CompilerParams(
                collective_id=0, has_side_effects=True, vmem_limit_bytes=room
            ),
        )(
            echoes, waveform, doppler_taper, cfar_guard, cfar_train, noise_floor,
            *(jnp.asarray(c) for c in consts),
        )
        return pl.pallas_call(
            write_kernel,
            out_shape=jax.ShapeDtypeStruct((1, beams, pulses, tiles * GB), f32),
            in_specs=[vmem],
            out_specs=hbm,
            scratch_shapes=[dma((beams, tiles))],
            compiler_params=pltpu.CompilerParams(vmem_limit_bytes=1024 * 1024),
        )(ratio)

    in_specs = (
        P(None, None, "groups", "shard", None),
        P(),
        P(),
        P("groups"),
        P("groups"),
        P("groups"),
    )
    return jax.shard_map(
        step, mesh=mesh, in_specs=in_specs, out_specs=P(None, "groups", None, "shard"), check_vma=False
    )
```

```python
import functools
import math

import jax
import jax.numpy as jnp
import numpy as np
from jax import lax
from jax.experimental import pallas as pl
from jax.experimental.pallas import tpu as pltpu
from jax.sharding import PartitionSpec as P

GB = 128
ROWS = 8
EDGE = 20
MESH = pl.DeviceIdType.MESH


def split(table):
    table = np.asarray(table, np.float32)
    high = table.astype(jnp.bfloat16)
    low = (table - high.astype(np.float32)).astype(jnp.bfloat16)
    return high, low


def dft(length, size=None):
    size = size or length
    i = np.arange(size)[:, None] * np.arange(length)[None, :] % length
    angles = 2.0 * np.pi / length * i
    return np.cos(angles), np.sin(angles)


def slots(tiles):
    return [0, tiles - 1, *range(tiles - 2, 0, -1)][:tiles]


def waiting(tiles):
    if tiles <= 2:
        return []
    j = slots(tiles)[-1]
    return [j, j - 1, j + 1]


def tables(gates, pulses, n):
    ga = gates // GB
    tiles = ga // n
    rows = (np.arange(0, ga, tiles)[:, None] + np.array(slots(tiles))[None, :]).reshape(-1)
    ca, sa = dft(ga)
    cb, sb = dft(GB)

    def left(matrix):
        high, low = split(matrix)
        return np.block([[high, high], [low, np.zeros_like(low)]])

    first = left(np.block([[ca, sa], [-sa, ca]]))
    last = left(np.block([[ca[rows], -sa[rows]], [sa[rows], ca[rows]]]))
    per = GB // ga
    c = np.arange(GB).reshape(GB // per, per).T.reshape(-1)
    cb, sb = cb[:, c], sb[:, c]
    second = np.stack(split(np.block([[cb, -sb], [sb, cb]])))
    third = np.stack(split(np.block([[cb.T, sb.T], [-sb.T, cb.T]])))
    i = np.arange(ga)[:, None] * np.arange(GB)[None, :] % gates
    twiddle = np.stack([np.cos(2 * np.pi / gates * i), np.sin(2 * np.pi / gates * i)])
    half = pulses // 2
    cp, sp = dft(pulses)
    doppler = [
        np.stack(split(np.concatenate([cp[e::2, :half], sp[e::2, :half]], axis=0))) for e in range(2)
    ]
    return np.stack([first, *second, *third, last]), twiddle.astype(np.float32), np.stack(doppler)


def parts(x):
    high = x.astype(jnp.bfloat16)
    low = (x - high.astype(jnp.float32)).astype(jnp.bfloat16)
    return high, low


def dot(a, b):
    return jnp.dot(a, b, preferred_element_type=jnp.float32)


def kernel(
    n, beams, pulses, gates,
    echoes, waveform_hbm, taper_hbm, guard_hbm, train_hbm, floor_hbm,
    chain_hbm, twiddle_hbm, doppler_hbm,
    out, num, den, over,
    xin, xs, wave, filt, sent, got, table, rhs, power, own, cross, edge, halo, band,
    waveform, taper, guard, train, floor, chain, twiddle,
    in_sem, small_sem, send_sem, recv_sem, edge_send, edge_recv,
):
    me = lax.axis_index("shard")
    ga = gates // GB
    tiles = ga // n
    groups = pulses // n // ROWS
    half = pulses // 2
    place = slots(tiles)
    outer = min(2, tiles)
    side = n // 2
    mine = lax.rem(me, side)
    far, here = side - (me - mine), me - mine
    across = [far + lax.rem(k + far // 2, side) for k in range(side)]
    near = [here + lax.rem(mine + k, side) for k in range(1, side)]
    order = across[:1] + [to for pair in zip(near, across[1:]) for to in pair]

    barrier = pltpu.get_barrier_semaphore()
    for to in order:
        pl.semaphore_signal(barrier, inc=1, device_id={"shard": to}, device_id_type=MESH)

    def load(b, start, size, sem):
        return pltpu.make_async_copy(
            echoes.at[0, :, b, pl.ds(start, size), :], xin.at[b, :, pl.ds(start, size)], in_sem.at[sem]
        )

    local = groups * ROWS
    loads = [load(0, 0, ROWS, beams)]
    loads += [load(0, ROWS, local - ROWS, 0)] if groups > 1 else []
    loads += [load(b, 0, local, b) for b in range(1, beams)]
    small = [
        pltpu.make_async_copy(src, dst, small_sem.at[i])
        for i, (src, dst) in enumerate(
            ((waveform_hbm, waveform), (chain_hbm, chain), (twiddle_hbm, twiddle), (taper_hbm, taper))
        )
    ]
    later = [
        pltpu.make_async_copy(src, dst, small_sem.at[i])
        for i, (src, dst) in enumerate(
            ((doppler_hbm, table), (guard_hbm, guard), (train_hbm, train), (floor_hbm, floor))
        )
    ]
    small[0].start()
    loads[0].start()
    for copy in small[1:]:
        copy.start()

    per = GB // ga
    scale = 1.0 / (gates * math.sqrt(pulses))
    small[0].wait()
    for c in range(2):
        for m in range(ga):
            wave[m:m + 1, :] = waveform[c:c + 1, m * GB:(m + 1) * GB]
        lines = wave[...] * scale
        turned = [lines] + [pltpu.roll(lines, GB - h * ga, axis=1) for h in range(1, per)]
        filt[c] = jnp.concatenate(turned, axis=0).T[:ga]
    def stage(i):
        return jnp.concatenate([chain[i], chain[i], chain[i + 1]], axis=0)

    def compress(b, pg):
        row = pg * ROWS if isinstance(pg, int) else pl.multiple_of(pg * ROWS, ROWS)
        for c in range(2):
            for i in range(ga):
                xs[c, i * ROWS:(i + 1) * ROWS, :] = xin[b, c, pl.ds(row, ROWS), i * GB:(i + 1) * GB]
        tc, ts = twiddle[0], twiddle[1]
        lhs = []
        for p in range(0, ROWS, 2):
            x = jnp.concatenate(
                [
                    jnp.concatenate([xs[c, pl.ds(p + e, ga, stride=ROWS), :] for c in range(2)], axis=0)
                    for e in range(2)
                ],
                axis=1,
            )
            y = dot(chain[0], jnp.concatenate(parts(x), axis=0))
            y = y[:2 * ga] + y[2 * ga:]
            for e in range(2):
                yr, yi = y[:ga, e * GB:(e + 1) * GB], y[ga:, e * GB:(e + 1) * GB]
                z = jnp.concatenate([yr * tc + yi * ts, yi * tc - yr * ts], axis=1)
                high, low = parts(z)
                lhs.append(jnp.concatenate([high, low, high], axis=1))
        x = dot(jnp.concatenate(lhs, axis=0), stage(1))
        lhs = []
        fr, fi = filt[0], filt[1]
        for p in range(ROWS):
            weight = taper[(me * groups + pg) * ROWS + p]
            hr, hi = fr * weight, fi * weight
            xr, xi = x[p * ga:(p + 1) * ga, :GB], x[p * ga:(p + 1) * ga, GB:]
            z = jnp.concatenate([xr * hr + xi * hi, xi * hr - xr * hi], axis=1)
            high, low = parts(z)
            lhs.append(jnp.concatenate([high, low, high], axis=1))
        x = dot(jnp.concatenate(lhs, axis=0), stage(3))
        for p in range(0, ROWS, 2):
            pair = []
            for e in range(2):
                r = (p + e) * ga
                xr, xi = x[r:r + ga, :GB], x[r:r + ga, GB:]
                pair.append(jnp.concatenate([xr * tc - xi * ts, xi * tc + xr * ts], axis=0))
            y = dot(chain[5], jnp.concatenate(parts(jnp.concatenate(pair, axis=1)), axis=0))
            y = y[:2 * ga] + y[2 * ga:]
            for e in range(2):
                for c in range(2):
                    sent.at[b, c, pg].reshape(ga * ROWS, GB)[pl.ds(p + e, ga, stride=ROWS), :] = y[
                        c * ga:(c + 1) * ga, e * GB:(e + 1) * GB
                    ]

    def send(src, dst, sem, peers, keep):
        for to in peers:
            pltpu.make_async_remote_copy(
                src_ref=src(to),
                dst_ref=dst,
                send_sem=send_sem,
                recv_sem=sem,
                device_id={"shard": to},
                device_id_type=MESH,
            ).start()
        if keep:
            pltpu.make_async_copy(src(me), dst, sem).start()

    def send_groups(b, pg, count):
        send(
            lambda to: sent.at[b, :, pl.ds(pg, count), pl.ds(to * tiles, outer)],
            got.at[b, :, pl.ds(me * groups + pg, count), pl.ds(0, outer)],
            recv_sem.at[b, 0], order, True,
        )

    def send_slot(b, t, peers, keep):
        send(
            lambda to: sent.at[b, :, :, to * tiles + t],
            got.at[b, :, pl.ds(me * groups, groups), t],
            recv_sem.at[b, t - outer + 1], peers, keep,
        )

    for copy in small[1:]:
        copy.wait()
    loads[0].wait()
    for copy in loads[1:2]:
        copy.start()
    compress(0, 0)
    pl.semaphore_wait(barrier, n - 1)
    send_groups(0, 0, 1)
    for copy in loads[2:] + later:
        copy.start()
    for b in range(beams):
        begin = 1 if b == 0 else 0
        if begin < groups:
            loads[b + 1 if groups > 1 else b].wait()

        @pl.loop(begin, groups)
        def _(pg):
            compress(b, pg)

            @pl.when(lax.rem(pg - begin, 2) == 1)
            def _():
                send_groups(b, pg - 1, 2)

            if (groups - begin) % 2:
                @pl.when(pg == groups - 1)
                def _():
                    send_groups(b, pg, 1)

    for t in range(outer, tiles - 1):
        for b in range(beams):
            send_slot(b, t, order, True)

    for copy in later:
        copy.wait()

    m = lax.broadcasted_iota(jnp.int32, (GB, 2 * GB), 0)
    k = lax.broadcasted_iota(jnp.int32, (GB, 2 * GB), 1)
    apart = jnp.where(k < GB, jnp.abs(m - k), jnp.where(k < GB + GB // 2, k - m, m + 2 * GB - k))
    for b in range(beams):
        inside = (apart > guard[b]) & (apart <= guard[b] + train[b])
        lines = jnp.where(inside, 1.0, 0.0).astype(jnp.bfloat16)
        band[b, :GB] = lines
        band[b, GB:] = lines

    def sums(b, x):
        return dot(jnp.concatenate(parts(x), axis=1), band[b])

    pending = waiting(tiles)

    def transform(b, t, final=False):
        j = place[t]
        x = jnp.concatenate([got[b, c, :, t].reshape(pulses, GB) for c in range(2)], axis=1)
        for e, y in enumerate((x[:half] + x[half:], x[:half] - x[half:])):
            high, low = parts(y)
            rhs[e, 0:half] = high
            rhs[e, half:2 * half] = low
            rhs[e, 2 * half:] = high
        for e in range(2):
            lhs = jnp.concatenate([table[e, 0], table[e, 0], table[e, 1]], axis=1)
            spec = dot(lhs, rhs[e])
            re = spec[:half, :GB] + spec[half:, GB:]
            im = spec[:half, GB:] - spec[half:, :GB]
            p = re * re + im * im
            power[b, j, e] = p
            total = sums(b, p)
            own[b, j, e] = total[:, :GB]
            cross[b, j + 1, e] = total[:, GB:]
            if final:
                over[e] = total[:, GB:]
                num[0, e] = p * scaled(b)
                den[0, e] = total[:, :GB] + den[0, e]

    def scaled(b):
        return 2.0 * train[b].astype(jnp.float32)

    def lower():
        return lax.broadcasted_iota(jnp.int32, (half, GB), 1) < GB // 2

    def ratio(b, j, e):
        total = own[b, j, e] + jnp.where(lower(), cross[b, j, e], cross[b, j + 2, e])
        out.at[b, j][pl.ds(e, half, stride=2), :] = (
            power[b, j, e] * scaled(b) / (floor[b] * scaled(b) + total)
        )

    def prepare(b, e):
        base = floor[b] * scaled(b)
        den[0, e] = jnp.where(lower(), cross[b, pending[0], e], cross[b, pending[0] + 2, e]) + base
        for i, j in enumerate(pending[1:], 1):
            num[i, e] = power[b, j, e] * scaled(b)
            part = jnp.where(lower(), cross[b, j, e], 0.0) if j < pending[0] else jnp.where(lower(), 0.0, cross[b, j + 2, e])
            den[i, e] = own[b, j, e] + part + base

    def send_edges(b):
        for side in range(2):
            cut = slice(0, EDGE) if side == 0 else slice(GB - EDGE, GB)
            for e in range(2):
                x = power[b, (tiles - 1) * side, e].T[cut]
                for i in range(half // GB):
                    start = (e * (half // GB) + i) * EDGE
                    edge[b, side, start:start + EDGE] = x[:, i * GB:(i + 1) * GB]
            pltpu.make_async_remote_copy(
                src_ref=edge.at[b, side],
                dst_ref=halo.at[b, side],
                send_sem=edge_send,
                recv_sem=edge_recv,
                device_id={"shard": lax.rem(me + (n - 1 if side == 0 else 1), n)},
                device_id_type=MESH,
            ).start()

    def take_edges():
        pltpu.make_async_copy(edge, edge, edge_send).wait()
        pltpu.make_async_copy(halo, halo, edge_recv).wait()
        zeros = jnp.zeros((GB - 2 * EDGE, half), jnp.float32)

        def lines(b, side, e):
            start = [(e * (half // GB) + i) * EDGE for i in range(half // GB)]
            x = jnp.concatenate([halo[b, side, i:i + EDGE] for i in start], axis=1)
            return jnp.where(me > 0 if side else me < n - 1, x, 0.0)

        for b in range(beams):
            for e in range(2):
                x = jnp.concatenate([lines(b, 0, e), zeros, lines(b, 1, e)], axis=0).T
                total = sums(b, x)[:, GB:]
                cross[b, 0, e] = total
                cross[b, tiles + 1, e] = total

    for b in range(beams):
        arrived = got.at[b, :, :, pl.ds(0, outer)]
        pltpu.make_async_copy(arrived, arrived, recv_sem.at[b, 0]).wait()
        for t in range(outer):
            transform(b, t)
        send_edges(b)

    if tiles > outer:
        for b in range(beams):
            send_slot(b, tiles - 1, near, True)
        for b in range(beams):
            send_slot(b, tiles - 1, across, False)

    done = [set() for _ in range(beams)]

    def ratios(b, ready, e):
        for j in range(tiles):
            if b == beams - 1 and j in pending:
                continue
            if j not in done[b] and {j - 1, j, j + 1} & set(range(tiles)) <= ready:
                ratio(b, j, e)
                if e == 1:
                    done[b].add(j)

    for t in range(outer, tiles):
        ready = set(place[:t + 1])
        for b in range(beams):
            final = t == tiles - 1 and b == beams - 1
            if final:
                if t == outer:
                    take_edges()
                for e in range(2):
                    prepare(b, e)
            arrived = got.at[b, :, :, t]
            pltpu.make_async_copy(arrived, arrived, recv_sem.at[b, t - outer + 1]).wait()
            transform(b, t, final)
            if t == tiles - 1 and not final and t > outer:
                for e in range(2):
                    ratios(b, ready, e)
        if t == tiles - 2:
            take_edges()
            for b in range(beams):
                for e in range(2):
                    ratios(b, ready, e)
    if tiles == outer:
        take_edges()
    if tiles <= outer + 1:
        for b in range(beams):
            for e in range(2):
                ratios(b, set(place), e)

    whole = sent.at[:, :, :, pl.ds(0, (n - 1) * tiles)]
    pltpu.make_async_copy(whole, whole, send_sem).wait()


def write_kernel(ratio, num, den, over, out, late, sem):
    beams, tiles = ratio.shape[:2]
    pending = waiting(tiles)
    half = num.shape[2]

    def put(b, j):
        i = pending.index(j) if b == beams - 1 and j in pending else None
        src = ratio.at[b, j] if i is None else late.at[i]
        return pltpu.make_async_copy(src, out.at[0, b, :, pl.ds(j * GB, GB)], sem)

    for b in range(beams):
        for j in range(tiles):
            if b < beams - 1 or j not in pending:
                put(b, j).start()
    lower = lax.broadcasted_iota(jnp.int32, (half, GB), 1) < GB // 2
    for i, j in enumerate(pending):
        for e in range(2):
            total = den[i, e]
            if i:
                total += jnp.where(lower == (j > pending[0]), over[e], 0.0)
            late.at[i][pl.ds(e, half, stride=2), :] = num[i, e] / total
        put(beams - 1, j).start()
    pltpu.make_async_copy(ratio, ratio, sem).wait()


def solution(mesh):
    n = mesh.shape["shard"]

    def step(echoes, waveform, doppler_taper, cfar_guard, cfar_train, noise_floor):
        beams, local, gates = echoes.shape[2:]
        pulses = local * n
        ga = gates // GB
        tiles = ga // n
        groups = local // ROWS
        half = pulses // 2
        consts = tables(gates, pulses, n)
        chain, twiddle, _ = consts
        vmem = pl.BlockSpec(memory_space=pltpu.VMEM)
        hbm = pl.BlockSpec(memory_space=pltpu.HBM)
        f32, bf16, i32 = jnp.float32, jnp.bfloat16, jnp.int32
        dma = pltpu.SemaphoreType.DMA
        late = max(1, len(waiting(tiles)))
        held = (
            (beams, tiles, pulses, GB), (late, 2, half, GB), (late, 2, half, GB), (2, half, GB),
        )
        room = 65456 * 1024 - sum(4 * math.prod(shape) for shape in held)
        results = pl.pallas_call(
            functools.partial(kernel, n, beams, pulses, gates),
            out_shape=tuple(pltpu.VMEM(shape, f32) for shape in held),
            in_specs=[hbm] * 9,
            out_specs=(vmem,) * 4,
            scratch_shapes=[
                pltpu.VMEM((beams, 2, local, gates), f32),
                pltpu.VMEM((2, ga * ROWS, GB), f32),
                pltpu.VMEM((ga, GB), f32),
                pltpu.VMEM((2, ga, GB), f32),
                pltpu.VMEM((beams, 2, groups, ga, ROWS, GB), f32),
                pltpu.VMEM((beams, 2, pulses // ROWS, tiles, ROWS, GB), f32),
                pltpu.VMEM((2, 2, pulses, half), bf16),
                pltpu.VMEM((2, 3 * half, 2 * GB), bf16),
                pltpu.VMEM((beams, tiles, 2, half, GB), f32),
                pltpu.VMEM((beams, tiles, 2, half, GB), f32),
                pltpu.VMEM((beams, tiles + 2, 2, half, GB), f32),
                pltpu.VMEM((beams, 2, pulses // GB * EDGE, GB), f32),
                pltpu.VMEM((beams, 2, pulses // GB * EDGE, GB), f32),
                pltpu.VMEM((beams, 2 * GB, 2 * GB), bf16),
                pltpu.VMEM((2, gates), f32),
                pltpu.SMEM((pulses,), f32),
                pltpu.SMEM((beams,), i32),
                pltpu.SMEM((beams,), i32),
                pltpu.SMEM((beams,), f32),
                pltpu.VMEM(chain.shape, bf16),
                pltpu.VMEM(twiddle.shape, f32),
                dma((beams + 1,)),
                dma((4,)),
                dma,
                dma((beams, tiles - min(2, tiles) + 1)),
                dma,
                dma,
            ],
            compiler_params=pltpu.CompilerParams(
                collective_id=0, has_side_effects=True, vmem_limit_bytes=room
            ),
        )(
            echoes, waveform, doppler_taper, cfar_guard, cfar_train, noise_floor,
            *(jnp.asarray(c) for c in consts),
        )
        return pl.pallas_call(
            write_kernel,
            out_shape=jax.ShapeDtypeStruct((1, beams, pulses, tiles * GB), f32),
            in_specs=[vmem] * 4,
            out_specs=hbm,
            scratch_shapes=[pltpu.VMEM((late, pulses, GB), f32), dma],
            compiler_params=pltpu.CompilerParams(vmem_limit_bytes=2048 * 1024),
        )(*results)

    in_specs = (
        P(None, None, "groups", "shard", None),
        P(),
        P(),
        P("groups"),
        P("groups"),
        P("groups"),
    )
    return jax.shard_map(
        step, mesh=mesh, in_specs=in_specs, out_specs=P(None, "groups", None, "shard"), check_vma=False
    )
```

```python
import functools
import math

import jax
import jax.numpy as jnp
import numpy as np
from jax import lax
from jax.experimental import pallas as pl
from jax.experimental.pallas import tpu as pltpu
from jax.sharding import PartitionSpec as P

GB = 128
ROWS = 8
EDGE = 20
RADIX = 4
MESH = pl.DeviceIdType.MESH


def split(table):
    table = np.asarray(table, np.float32)
    high = table.astype(jnp.bfloat16)
    low = (table - high.astype(np.float32)).astype(jnp.bfloat16)
    return high, low


def dft(length, size=None):
    size = size or length
    i = np.arange(size)[:, None] * np.arange(length)[None, :] % length
    angles = 2.0 * np.pi / length * i
    return np.cos(angles), np.sin(angles)


def slots(tiles):
    return [0, tiles - 1, *range(tiles - 2, 0, -1)][:tiles]


def waiting(tiles):
    if tiles <= 2:
        return []
    j = slots(tiles)[-1]
    return [j, j - 1, j + 1]


def tables(gates, pulses, n):
    ga = gates // GB
    tiles = ga // n
    rows = (np.arange(0, ga, tiles)[:, None] + np.array(slots(tiles))[None, :]).reshape(-1)
    ca, sa = dft(ga)
    cb, sb = dft(GB)

    def left(matrix):
        high, low = split(matrix)
        return np.block([[high, high], [low, np.zeros_like(low)]])

    first = left(np.block([[ca, sa], [-sa, ca]]))
    last = left(np.block([[ca[rows], -sa[rows]], [sa[rows], ca[rows]]]))
    per = GB // ga
    c = np.arange(GB).reshape(GB // per, per).T.reshape(-1)
    cb, sb = cb[:, c], sb[:, c]
    second = np.stack(split(np.block([[cb, -sb], [sb, cb]])))
    third = np.stack(split(np.block([[cb.T, sb.T], [-sb.T, cb.T]])))
    i = np.arange(ga)[:, None] * np.arange(GB)[None, :] % gates
    twiddle = np.stack([np.cos(2 * np.pi / gates * i), np.sin(2 * np.pi / gates * i)])
    part = pulses // RADIX
    cp, sp = dft(pulses)
    doppler = [
        np.stack(split(np.concatenate([cp[e::RADIX, :part], sp[e::RADIX, :part]], axis=0)))
        for e in range(RADIX)
    ]
    return np.stack([first, *second, *third, last]), twiddle.astype(np.float32), np.stack(doppler)


def parts(x):
    high = x.astype(jnp.bfloat16)
    low = (x - high.astype(jnp.float32)).astype(jnp.bfloat16)
    return high, low


def dot(a, b):
    return jnp.dot(a, b, preferred_element_type=jnp.float32)


def rotated(x):
    if len(x) == 2:
        return [[p + q for p, q in zip(*x)], [p - q for p, q in zip(*x)]]
    (ar, ai), (br, bi), (cr, ci), (dr, di) = x
    sr, si, tr, ti = ar + cr, ai + ci, ar - cr, ai - ci
    ur, ui, vr, vi = br + dr, bi + di, br - dr, bi - di
    return [(sr + ur, si + ui), (tr + vi, ti - vr), (sr - ur, si - ui), (tr - vi, ti + vr)]


def stacked(high, low, axis):
    return jnp.concatenate([high, high, low] if axis else [high, low, high], axis=axis)


def intensity(table, high, low):
    spec = dot(stacked(table[0], table[1], 1), stacked(high, low, 0))
    part = spec.shape[0] // 2
    re = spec[:part, :GB] + spec[part:, GB:]
    im = spec[:part, GB:] - spec[part:, :GB]
    return re * re + im * im


def sums(x, band):
    return dot(jnp.concatenate(parts(x), axis=1), band)


def kernel(
    n, beams, pulses, gates,
    echoes, waveform_hbm, taper_hbm, guard_hbm, train_hbm, floor_hbm,
    chain_hbm, twiddle_hbm, doppler_hbm,
    out, num, den, tail, table, sieve, factor,
    xin, xs, wave, filt, sent, got, rhs, power, own, cross, edge, halo, band,
    waveform, taper, guard, train, floor, chain, twiddle,
    in_sem, small_sem, send_sem, recv_sem, edge_send, edge_recv,
):
    me = lax.axis_index("shard")
    ga = gates // GB
    tiles = ga // n
    groups = pulses // n // ROWS
    part = pulses // RADIX
    place = slots(tiles)
    outer = min(2, tiles)
    side = n // 2
    mine = lax.rem(me, side)
    far, here = side - (me - mine), me - mine
    across = [far + k for k in range(side)]
    near = [here + lax.rem(mine + k, side) for k in range(1, side)]
    order = across[:1] + [to for pair in zip(near, across[1:]) for to in pair]

    barrier = pltpu.get_barrier_semaphore()
    for to in order:
        pl.semaphore_signal(barrier, inc=1, device_id={"shard": to}, device_id_type=MESH)

    def load(b, start, size, sem):
        return pltpu.make_async_copy(
            echoes.at[0, :, b, pl.ds(start, size), :], xin.at[b, :, pl.ds(start, size)], in_sem.at[sem]
        )

    local = groups * ROWS
    loads = [load(0, 0, ROWS, beams)]
    loads += [load(0, ROWS, local - ROWS, 0)] if groups > 1 else []
    loads += [load(b, 0, local, b) for b in range(1, beams)]
    small = [
        pltpu.make_async_copy(src, dst, small_sem.at[i])
        for i, (src, dst) in enumerate(
            ((waveform_hbm, waveform), (chain_hbm, chain), (twiddle_hbm, twiddle), (taper_hbm, taper))
        )
    ]
    later = [
        pltpu.make_async_copy(src, dst, small_sem.at[i])
        for i, (src, dst) in enumerate(
            ((doppler_hbm, table), (guard_hbm, guard), (train_hbm, train), (floor_hbm, floor))
        )
    ]
    small[0].start()
    loads[0].start()
    for copy in small[1:]:
        copy.start()

    per = GB // ga
    scale = 1.0 / (gates * math.sqrt(pulses))
    small[0].wait()
    for c in range(2):
        for m in range(ga):
            wave[m:m + 1, :] = waveform[c:c + 1, m * GB:(m + 1) * GB]
        lines = wave[...] * scale
        turned = [lines] + [pltpu.roll(lines, GB - h * ga, axis=1) for h in range(1, per)]
        filt[c] = jnp.concatenate(turned, axis=0).T[:ga]
    def stage(i):
        return jnp.concatenate([chain[i], chain[i], chain[i + 1]], axis=0)

    def compress(b, pg):
        row = pg * ROWS if isinstance(pg, int) else pl.multiple_of(pg * ROWS, ROWS)
        for c in range(2):
            for i in range(ga):
                xs[c, i * ROWS:(i + 1) * ROWS, :] = xin[b, c, pl.ds(row, ROWS), i * GB:(i + 1) * GB]
        tc, ts = twiddle[0], twiddle[1]
        lhs = []
        for p in range(0, ROWS, 2):
            x = jnp.concatenate(
                [
                    jnp.concatenate([xs[c, pl.ds(p + e, ga, stride=ROWS), :] for c in range(2)], axis=0)
                    for e in range(2)
                ],
                axis=1,
            )
            y = dot(chain[0], jnp.concatenate(parts(x), axis=0))
            y = y[:2 * ga] + y[2 * ga:]
            for e in range(2):
                yr, yi = y[:ga, e * GB:(e + 1) * GB], y[ga:, e * GB:(e + 1) * GB]
                z = jnp.concatenate([yr * tc + yi * ts, yi * tc - yr * ts], axis=1)
                high, low = parts(z)
                lhs.append(jnp.concatenate([high, low, high], axis=1))
        x = dot(jnp.concatenate(lhs, axis=0), stage(1))
        lhs = []
        fr, fi = filt[0], filt[1]
        for p in range(ROWS):
            weight = taper[(me * groups + pg) * ROWS + p]
            hr, hi = fr * weight, fi * weight
            xr, xi = x[p * ga:(p + 1) * ga, :GB], x[p * ga:(p + 1) * ga, GB:]
            z = jnp.concatenate([xr * hr + xi * hi, xi * hr - xr * hi], axis=1)
            high, low = parts(z)
            lhs.append(jnp.concatenate([high, low, high], axis=1))
        x = dot(jnp.concatenate(lhs, axis=0), stage(3))
        for p in range(0, ROWS, 2):
            pair = []
            for e in range(2):
                r = (p + e) * ga
                xr, xi = x[r:r + ga, :GB], x[r:r + ga, GB:]
                pair.append(jnp.concatenate([xr * tc - xi * ts, xi * tc + xr * ts], axis=0))
            y = dot(chain[5], jnp.concatenate(parts(jnp.concatenate(pair, axis=1)), axis=0))
            y = y[:2 * ga] + y[2 * ga:]
            for e in range(2):
                for c in range(2):
                    sent.at[b, c, pg].reshape(ga * ROWS, GB)[pl.ds(p + e, ga, stride=ROWS), :] = y[
                        c * ga:(c + 1) * ga, e * GB:(e + 1) * GB
                    ]

    def send(src, dst, sem, peers, keep):
        for to in peers:
            pltpu.make_async_remote_copy(
                src_ref=src(to),
                dst_ref=dst,
                send_sem=send_sem,
                recv_sem=sem,
                device_id={"shard": to},
                device_id_type=MESH,
            ).start()
        if keep:
            pltpu.make_async_copy(src(me), dst, sem).start()

    def send_groups(b, pg, count):
        send(
            lambda to: sent.at[b, :, pl.ds(pg, count), pl.ds(to * tiles, outer)],
            got.at[b, :, pl.ds(me * groups + pg, count), pl.ds(0, outer)],
            recv_sem.at[b, 0], order, True,
        )

    def send_slot(b, t, peers, keep):
        send(
            lambda to: sent.at[b, :, :, to * tiles + t],
            got.at[b, :, pl.ds(me * groups, groups), t],
            recv_sem.at[b, t - outer + 1], peers, keep,
        )

    for copy in small[1:]:
        copy.wait()
    loads[0].wait()
    for copy in loads[1:2]:
        copy.start()
    compress(0, 0)
    pl.semaphore_wait(barrier, n - 1)
    send_groups(0, 0, 1)
    for copy in loads[2:] + later:
        copy.start()
    for b in range(beams):
        begin = 1 if b == 0 else 0
        if begin < groups:
            loads[b + 1 if groups > 1 else b].wait()

        @pl.loop(begin, groups)
        def _(pg):
            compress(b, pg)

            @pl.when(lax.rem(pg - begin, 2) == 1)
            def _():
                send_groups(b, pg - 1, 2)

            if (groups - begin) % 2:
                @pl.when(pg == groups - 1)
                def _():
                    send_groups(b, pg, 1)

    for t in range(outer, tiles - 1):
        for b in range(beams):
            send_slot(b, t, order, True)

    for copy in later:
        copy.wait()

    m = lax.broadcasted_iota(jnp.int32, (GB, 2 * GB), 0)
    k = lax.broadcasted_iota(jnp.int32, (GB, 2 * GB), 1)
    apart = jnp.where(k < GB, jnp.abs(m - k), jnp.where(k < GB + GB // 2, k - m, m + 2 * GB - k))
    for b in range(beams):
        inside = (apart > guard[b]) & (apart <= guard[b] + train[b])
        lines = jnp.where(inside, 1.0, 0.0).astype(jnp.bfloat16)
        band[b, :GB] = lines
        band[b, GB:] = lines

    pending = waiting(tiles)

    def branches(b, t):
        x = [got[b, c, :, t].reshape(RADIX, part, GB) for c in range(2)]
        return [parts(jnp.concatenate(y, axis=1)) for y in rotated([(x[0][i], x[1][i]) for i in range(RADIX)])]

    def transform(b, t):
        j = place[t]
        for e, (high, low) in enumerate(branches(b, t)):
            rhs[e, 0] = high
            rhs[e, 1] = low
        for e in range(RADIX):
            p = intensity(table.at[e], rhs[e, 0], rhs[e, 1])
            power[b, j, e] = p
            total = sums(p, band[b])
            own[b, j, e] = total[:, :GB]
            cross[b, j + 1, e] = total[:, GB:]

    def scaled(b):
        return 2.0 * train[b].astype(jnp.float32)

    def lower():
        return lax.broadcasted_iota(jnp.int32, (part, GB), 1) < GB // 2

    def ratio(b, j, e):
        total = own[b, j, e] + jnp.where(lower(), cross[b, j, e], cross[b, j + 2, e])
        out.at[b, j][pl.ds(e, part, stride=RADIX), :] = (
            power[b, j, e] * scaled(b) / (floor[b] * scaled(b) + total)
        )

    def prepare(b, e):
        base = floor[b] * scaled(b)
        den[0, e] = jnp.where(lower(), cross[b, pending[0], e], cross[b, pending[0] + 2, e]) + base
        for i, j in enumerate(pending[1:], 1):
            num[i, e] = power[b, j, e] * scaled(b)
            beside = cross[b, j, e] if j < pending[0] else cross[b, j + 2, e]
            den[i, e] = own[b, j, e] + jnp.where(lower() == (j < pending[0]), beside, 0.0) + base

    def send_edges(b):
        for side in range(2):
            cut = slice(0, EDGE) if side == 0 else slice(GB - EDGE, GB)
            for e in range(RADIX):
                x = power[b, (tiles - 1) * side, e].T[cut]
                for i in range(part // GB):
                    start = (e * (part // GB) + i) * EDGE
                    edge[b, side, start:start + EDGE] = x[:, i * GB:(i + 1) * GB]
            pltpu.make_async_remote_copy(
                src_ref=edge.at[b, side],
                dst_ref=halo.at[b, side],
                send_sem=edge_send,
                recv_sem=edge_recv,
                device_id={"shard": lax.rem(me + (n - 1 if side == 0 else 1), n)},
                device_id_type=MESH,
            ).start()

    def take_edges():
        pltpu.make_async_copy(edge, edge, edge_send).wait()
        pltpu.make_async_copy(halo, halo, edge_recv).wait()
        zeros = jnp.zeros((GB - 2 * EDGE, part), jnp.float32)

        def lines(b, side, e):
            start = [(e * (part // GB) + i) * EDGE for i in range(part // GB)]
            x = jnp.concatenate([halo[b, side, i:i + EDGE] for i in start], axis=1)
            return jnp.where(me > 0 if side else me < n - 1, x, 0.0)

        for b in range(beams):
            for e in range(RADIX):
                x = jnp.concatenate([lines(b, 0, e), zeros, lines(b, 1, e)], axis=0).T
                total = sums(x, band[b])[:, GB:]
                cross[b, 0, e] = total
                cross[b, tiles + 1, e] = total

    for b in range(beams):
        arrived = got.at[b, :, :, pl.ds(0, outer)]
        pltpu.make_async_copy(arrived, arrived, recv_sem.at[b, 0]).wait()
        for t in range(outer):
            transform(b, t)
        send_edges(b)

    if tiles > outer:
        for b in range(beams):
            send_slot(b, tiles - 1, near, True)
        for b in range(beams):
            send_slot(b, tiles - 1, across, False)

    done = [set() for _ in range(beams)]

    def ratios(b, ready):
        for j in range(tiles):
            if b == beams - 1 and j in pending:
                continue
            if j not in done[b] and {j - 1, j, j + 1} & set(range(tiles)) <= ready:
                for e in range(RADIX):
                    ratio(b, j, e)
                done[b].add(j)

    for t in range(outer, tiles):
        ready = set(place[:t + 1])
        for b in range(beams):
            final = t == tiles - 1 and b == beams - 1
            if final:
                if t == outer:
                    take_edges()
                    for i in range(beams - 1):
                        ratios(i, ready)
                for e in range(RADIX):
                    prepare(b, e)
                sieve[...] = band[b]
                factor[...] = jnp.full(factor.shape, scaled(b))
            arrived = got.at[b, :, :, t]
            pltpu.make_async_copy(arrived, arrived, recv_sem.at[b, t - outer + 1]).wait()
            if final:
                for e, (high, low) in enumerate(branches(b, t)):
                    tail[e, 0] = high
                    tail[e, 1] = low
                continue
            transform(b, t)
            if t == tiles - 1 and t > outer:
                ratios(b, ready)
        if t == tiles - 2:
            take_edges()
            for b in range(beams):
                ratios(b, ready)
    if tiles == outer:
        take_edges()
        for b in range(beams):
            ratios(b, set(place))

    whole = sent.at[:, :, :, pl.ds(0, (n - 1) * tiles)]
    pltpu.make_async_copy(whole, whole, send_sem).wait()


def write_kernel(ratio, num, den, tail, table, sieve, factor, out, late, pw, sem):
    beams, tiles = ratio.shape[:2]
    pending = waiting(tiles)
    part = num.shape[2]

    def put(b, j):
        i = pending.index(j) if b == beams - 1 and j in pending else None
        src = ratio.at[b, j] if i is None else late.at[i]
        return pltpu.make_async_copy(src, out.at[0, b, :, pl.ds(j * GB, GB)], sem)

    for b in range(beams):
        for j in range(tiles):
            if b < beams - 1 or j not in pending:
                put(b, j).start()
    lower = lax.broadcasted_iota(jnp.int32, (part, GB), 1) < GB // 2
    if pending:
        for e in range(RADIX):
            pw[e] = intensity(table.at[e], tail[e, 0], tail[e, 1])

        for e in range(RADIX):
            p = pw[e]
            total = sums(p, sieve[...])
            for i, j in enumerate(pending):
                if i:
                    add = jnp.where(lower == (j > pending[0]), total[:, GB:], 0.0)
                else:
                    add = total[:, :GB]
                top = num[i, e] if i else p * factor[0:1]
                late.at[i][pl.ds(e, part, stride=RADIX), :] = top / (den[i, e] + add)
    for j in pending:
        put(beams - 1, j).start()
    pltpu.make_async_copy(ratio, ratio, sem).wait()


def solution(mesh):
    n = mesh.shape["shard"]

    def step(echoes, waveform, doppler_taper, cfar_guard, cfar_train, noise_floor):
        beams, local, gates = echoes.shape[2:]
        pulses = local * n
        ga = gates // GB
        tiles = ga // n
        groups = local // ROWS
        part = pulses // RADIX
        consts = tables(gates, pulses, n)
        chain, twiddle, _ = consts
        vmem = pl.BlockSpec(memory_space=pltpu.VMEM)
        hbm = pl.BlockSpec(memory_space=pltpu.HBM)
        f32, bf16, i32 = jnp.float32, jnp.bfloat16, jnp.int32
        dma = pltpu.SemaphoreType.DMA
        late = max(1, len(waiting(tiles)))
        held = [
            pltpu.VMEM(*x)
            for x in (
                ((beams, tiles, pulses, GB), f32), ((late, RADIX, part, GB), f32),
                ((late, RADIX, part, GB), f32), ((RADIX, 2, part, 2 * GB), bf16),
                ((RADIX, 2, 2 * part, part), bf16), ((2 * GB, 2 * GB), bf16), ((8, GB), f32),
            )
        ]
        room = 65456 * 1024 - sum(x.dtype.itemsize * math.prod(x.shape) for x in held)
        results = pl.pallas_call(
            functools.partial(kernel, n, beams, pulses, gates),
            out_shape=tuple(held),
            in_specs=[hbm] * 9,
            out_specs=(vmem,) * len(held),
            scratch_shapes=[
                pltpu.VMEM((beams, 2, local, gates), f32),
                pltpu.VMEM((2, ga * ROWS, GB), f32),
                pltpu.VMEM((ga, GB), f32),
                pltpu.VMEM((2, ga, GB), f32),
                pltpu.VMEM((beams, 2, groups, ga, ROWS, GB), f32),
                pltpu.VMEM((beams, 2, pulses // ROWS, tiles, ROWS, GB), f32),
                pltpu.VMEM((RADIX, 2, part, 2 * GB), bf16),
                pltpu.VMEM((beams, tiles, RADIX, part, GB), f32),
                pltpu.VMEM((beams, tiles, RADIX, part, GB), f32),
                pltpu.VMEM((beams, tiles + 2, RADIX, part, GB), f32),
                pltpu.VMEM((beams, 2, pulses // GB * EDGE, GB), f32),
                pltpu.VMEM((beams, 2, pulses // GB * EDGE, GB), f32),
                pltpu.VMEM((beams, 2 * GB, 2 * GB), bf16),
                pltpu.VMEM((2, gates), f32),
                pltpu.SMEM((pulses,), f32),
                pltpu.SMEM((beams,), i32),
                pltpu.SMEM((beams,), i32),
                pltpu.SMEM((beams,), f32),
                pltpu.VMEM(chain.shape, bf16),
                pltpu.VMEM(twiddle.shape, f32),
                dma((beams + 1,)),
                dma((4,)),
                dma,
                dma((beams, tiles - min(2, tiles) + 1)),
                dma,
                dma,
            ],
            compiler_params=pltpu.CompilerParams(
                collective_id=0, has_side_effects=True, vmem_limit_bytes=room
            ),
        )(
            echoes, waveform, doppler_taper, cfar_guard, cfar_train, noise_floor,
            *(jnp.asarray(c) for c in consts),
        )
        return pl.pallas_call(
            write_kernel,
            out_shape=jax.ShapeDtypeStruct((1, beams, pulses, tiles * GB), f32),
            in_specs=[vmem] * len(held),
            out_specs=hbm,
            scratch_shapes=[pltpu.VMEM((late, pulses, GB), f32), pltpu.VMEM((RADIX, part, GB), f32), dma],
            compiler_params=pltpu.CompilerParams(vmem_limit_bytes=4096 * 1024),
        )(*results)

    in_specs = (
        P(None, None, "groups", "shard", None),
        P(),
        P(),
        P("groups"),
        P("groups"),
        P("groups"),
    )
    return jax.shard_map(
        step, mesh=mesh, in_specs=in_specs, out_specs=P(None, "groups", None, "shard"), check_vma=False
    )
```

```python
import functools
import math

import jax
import jax.numpy as jnp
import numpy as np
from jax import lax
from jax.experimental import pallas as pl
from jax.experimental.pallas import tpu as pltpu
from jax.sharding import PartitionSpec as P

GB = 128
ROWS = 8
EDGE = 20
RADIX = 4
MESH = pl.DeviceIdType.MESH


def split(table):
    table = np.asarray(table, np.float32)
    high = table.astype(jnp.bfloat16)
    low = (table - high.astype(np.float32)).astype(jnp.bfloat16)
    return high, low


def dft(length, size=None):
    size = size or length
    i = np.arange(size)[:, None] * np.arange(length)[None, :] % length
    angles = 2.0 * np.pi / length * i
    return np.cos(angles), np.sin(angles)


def slots(tiles):
    return [0, tiles - 1, *range(tiles - 2, 0, -1)][:tiles]


def waiting(tiles):
    if tiles <= 2:
        return []
    j = slots(tiles)[-1]
    return [j, j - 1, j + 1]


def tables(gates, pulses, n):
    ga = gates // GB
    tiles = ga // n
    rows = (np.arange(0, ga, tiles)[:, None] + np.array(slots(tiles))[None, :]).reshape(-1)
    ca, sa = dft(ga)
    cb, sb = dft(GB)

    def left(matrix):
        high, low = split(matrix)
        return np.block([[high, high], [low, np.zeros_like(low)]])

    first = left(np.block([[ca, sa], [-sa, ca]]))
    last = left(np.block([[ca[rows], -sa[rows]], [sa[rows], ca[rows]]]))
    per = GB // ga
    c = np.arange(GB).reshape(GB // per, per).T.reshape(-1)
    cb, sb = cb[:, c], sb[:, c]
    second = np.stack(split(np.block([[cb, -sb], [sb, cb]])))
    third = np.stack(split(np.block([[cb.T, sb.T], [-sb.T, cb.T]])))
    i = np.arange(ga)[:, None] * np.arange(GB)[None, :] % gates
    twiddle = np.stack([np.cos(2 * np.pi / gates * i), np.sin(2 * np.pi / gates * i)])
    part = pulses // RADIX
    cp, sp = dft(pulses)
    doppler = [
        np.stack(split(np.concatenate([cp[e::RADIX, :part], sp[e::RADIX, :part]], axis=0)))
        for e in range(RADIX)
    ]
    return np.stack([first, *second, *third, last]), twiddle.astype(np.float32), np.stack(doppler)


def parts(x):
    high = x.astype(jnp.bfloat16)
    low = (x - high.astype(jnp.float32)).astype(jnp.bfloat16)
    return high, low


def dot(a, b):
    return jnp.dot(a, b, preferred_element_type=jnp.float32)


def rotated(x):
    if len(x) == 2:
        return [[p + q for p, q in zip(*x)], [p - q for p, q in zip(*x)]]
    (ar, ai), (br, bi), (cr, ci), (dr, di) = x
    sr, si, tr, ti = ar + cr, ai + ci, ar - cr, ai - ci
    ur, ui, vr, vi = br + dr, bi + di, br - dr, bi - di
    return [(sr + ur, si + ui), (tr + vi, ti - vr), (sr - ur, si - ui), (tr - vi, ti + vr)]


def stacked(high, low, axis):
    return jnp.concatenate([high, high, low] if axis else [high, low, high], axis=axis)


def intensity(table, high, low):
    spec = dot(stacked(table[0], table[1], 1), stacked(high, low, 0))
    part = spec.shape[0] // 2
    re = spec[:part, :GB] + spec[part:, GB:]
    im = spec[:part, GB:] - spec[part:, :GB]
    return re * re + im * im


def sums(x, band):
    return dot(jnp.concatenate(parts(x), axis=1), band)


def kernel(
    n, beams, pulses, gates,
    echoes, waveform_hbm, taper_hbm, guard_hbm, train_hbm, floor_hbm,
    chain_hbm, twiddle_hbm, doppler_hbm,
    out, num, den, tail, table, sieve, factor,
    xin, xs, wave, filt, sent, got, rhs, power, own, cross, edge, halo, relay, band,
    waveform, taper, guard, train, floor, chain, twiddle,
    in_sem, small_sem, send_sem, recv_sem, edge_send, edge_recv, relay_sem,
):
    me = lax.axis_index("shard")
    ga = gates // GB
    tiles = ga // n
    groups = pulses // n // ROWS
    part = pulses // RADIX
    place = slots(tiles)
    outer = min(2, tiles)
    side = n // 2
    mine = lax.rem(me, side)
    far, here = side - (me - mine), me - mine
    across = [far + k for k in range(side)]
    near = [here + lax.rem(mine + k, side) for k in range(1, side)]
    order = across[:1] + [to for pair in zip(near, across[1:]) for to in pair]

    barrier = pltpu.get_barrier_semaphore()
    for to in order:
        pl.semaphore_signal(barrier, inc=1, device_id={"shard": to}, device_id_type=MESH)

    def load(b, start, size, sem):
        return pltpu.make_async_copy(
            echoes.at[0, :, b, pl.ds(start, size), :], xin.at[b, :, pl.ds(start, size)], in_sem.at[sem]
        )

    local = groups * ROWS
    loads = [load(0, 0, ROWS, beams)]
    loads += [load(0, ROWS, local - ROWS, 0)] if groups > 1 else []
    loads += [load(b, 0, local, b) for b in range(1, beams)]
    small = [
        pltpu.make_async_copy(src, dst, small_sem.at[i])
        for i, (src, dst) in enumerate(
            ((waveform_hbm, waveform), (chain_hbm, chain), (twiddle_hbm, twiddle), (taper_hbm, taper))
        )
    ]
    later = [
        pltpu.make_async_copy(src, dst, small_sem.at[i])
        for i, (src, dst) in enumerate(
            ((doppler_hbm, table), (guard_hbm, guard), (train_hbm, train), (floor_hbm, floor))
        )
    ]
    small[0].start()
    loads[0].start()
    for copy in small[1:]:
        copy.start()

    per = GB // ga
    scale = 1.0 / (gates * math.sqrt(pulses))
    small[0].wait()
    for c in range(2):
        for m in range(ga):
            wave[m:m + 1, :] = waveform[c:c + 1, m * GB:(m + 1) * GB]
        lines = wave[...] * scale
        turned = [lines] + [pltpu.roll(lines, GB - h * ga, axis=1) for h in range(1, per)]
        filt[c] = jnp.concatenate(turned, axis=0).T[:ga]
    def stage(i):
        return jnp.concatenate([chain[i], chain[i], chain[i + 1]], axis=0)

    def compress(b, pg):
        row = pg * ROWS if isinstance(pg, int) else pl.multiple_of(pg * ROWS, ROWS)
        for c in range(2):
            for i in range(ga):
                xs[c, i * ROWS:(i + 1) * ROWS, :] = xin[b, c, pl.ds(row, ROWS), i * GB:(i + 1) * GB]
        tc, ts = twiddle[0], twiddle[1]
        lhs = []
        for p in range(0, ROWS, 2):
            x = jnp.concatenate(
                [
                    jnp.concatenate([xs[c, pl.ds(p + e, ga, stride=ROWS), :] for c in range(2)], axis=0)
                    for e in range(2)
                ],
                axis=1,
            )
            y = dot(chain[0], jnp.concatenate(parts(x), axis=0))
            y = y[:2 * ga] + y[2 * ga:]
            for e in range(2):
                yr, yi = y[:ga, e * GB:(e + 1) * GB], y[ga:, e * GB:(e + 1) * GB]
                z = jnp.concatenate([yr * tc + yi * ts, yi * tc - yr * ts], axis=1)
                high, low = parts(z)
                lhs.append(jnp.concatenate([high, low, high], axis=1))
        x = dot(jnp.concatenate(lhs, axis=0), stage(1))
        lhs = []
        fr, fi = filt[0], filt[1]
        for p in range(ROWS):
            weight = taper[(me * groups + pg) * ROWS + p]
            hr, hi = fr * weight, fi * weight
            xr, xi = x[p * ga:(p + 1) * ga, :GB], x[p * ga:(p + 1) * ga, GB:]
            z = jnp.concatenate([xr * hr + xi * hi, xi * hr - xr * hi], axis=1)
            high, low = parts(z)
            lhs.append(jnp.concatenate([high, low, high], axis=1))
        x = dot(jnp.concatenate(lhs, axis=0), stage(3))
        for p in range(0, ROWS, 2):
            pair = []
            for e in range(2):
                r = (p + e) * ga
                xr, xi = x[r:r + ga, :GB], x[r:r + ga, GB:]
                pair.append(jnp.concatenate([xr * tc - xi * ts, xi * tc + xr * ts], axis=0))
            y = dot(chain[5], jnp.concatenate(parts(jnp.concatenate(pair, axis=1)), axis=0))
            y = y[:2 * ga] + y[2 * ga:]
            for e in range(2):
                for c in range(2):
                    sent.at[b, c, pg].reshape(ga * ROWS, GB)[pl.ds(p + e, ga, stride=ROWS), :] = y[
                        c * ga:(c + 1) * ga, e * GB:(e + 1) * GB
                    ]

    def send(src, dst, sem, peers, keep):
        for to in peers:
            pltpu.make_async_remote_copy(
                src_ref=src(to),
                dst_ref=dst,
                send_sem=send_sem,
                recv_sem=sem,
                device_id={"shard": to},
                device_id_type=MESH,
            ).start()
        if keep:
            pltpu.make_async_copy(src(me), dst, sem).start()

    def send_groups(b, pg, count):
        send(
            lambda to: sent.at[b, :, pl.ds(pg, count), pl.ds(to * tiles, outer)],
            got.at[b, :, pl.ds(me * groups + pg, count), pl.ds(0, outer)],
            recv_sem.at[b, 0], order, True,
        )

    def send_slot(b, t, peers, keep):
        send(
            lambda to: sent.at[b, :, :, to * tiles + t],
            got.at[b, :, pl.ds(me * groups, groups), t],
            recv_sem.at[b, t - outer + 1], peers, keep,
        )

    for copy in small[1:]:
        copy.wait()
    loads[0].wait()
    for copy in loads[1:2]:
        copy.start()
    compress(0, 0)
    pl.semaphore_wait(barrier, n - 1)
    send_groups(0, 0, 1)
    for copy in loads[2:] + later:
        copy.start()
    for b in range(beams):
        begin = 1 if b == 0 else 0
        if begin < groups:
            loads[b + 1 if groups > 1 else b].wait()

        @pl.loop(begin, groups)
        def _(pg):
            compress(b, pg)

            @pl.when(lax.rem(pg - begin, 2) == 1)
            def _():
                send_groups(b, pg - 1, 2)

            if (groups - begin) % 2:
                @pl.when(pg == groups - 1)
                def _():
                    send_groups(b, pg, 1)

    for t in range(outer, tiles - 1):
        for b in range(beams):
            send_slot(b, t, order, True)

    for copy in later:
        copy.wait()

    m = lax.broadcasted_iota(jnp.int32, (GB, 2 * GB), 0)
    k = lax.broadcasted_iota(jnp.int32, (GB, 2 * GB), 1)
    apart = jnp.where(k < GB, jnp.abs(m - k), jnp.where(k < GB + GB // 2, k - m, m + 2 * GB - k))
    for b in range(beams):
        inside = (apart > guard[b]) & (apart <= guard[b] + train[b])
        lines = jnp.where(inside, 1.0, 0.0).astype(jnp.bfloat16)
        band[b, :GB] = lines
        band[b, GB:] = lines

    pending = waiting(tiles)

    def branches(b, t):
        x = [got[b, c, :, t].reshape(RADIX, part, GB) for c in range(2)]
        return [parts(jnp.concatenate(y, axis=1)) for y in rotated([(x[0][i], x[1][i]) for i in range(RADIX)])]

    def transform(b, t):
        j = place[t]
        for e, (high, low) in enumerate(branches(b, t)):
            rhs[e, 0] = high
            rhs[e, 1] = low
        for e in range(RADIX):
            p = intensity(table.at[e], rhs[e, 0], rhs[e, 1])
            power[b, j, e] = p
            total = sums(p, band[b])
            own[b, j, e] = total[:, :GB]
            cross[b, j + 1, e] = total[:, GB:]

    def scaled(b):
        return 2.0 * train[b].astype(jnp.float32)

    def lower():
        return lax.broadcasted_iota(jnp.int32, (part, GB), 1) < GB // 2

    def ratio(b, j, e):
        total = own[b, j, e] + jnp.where(lower(), cross[b, j, e], cross[b, j + 2, e])
        out.at[b, j][pl.ds(e, part, stride=RADIX), :] = (
            power[b, j, e] * scaled(b) / (floor[b] * scaled(b) + total)
        )

    def prepare(b, e):
        base = floor[b] * scaled(b)
        den[0, e] = jnp.where(lower(), cross[b, pending[0], e], cross[b, pending[0] + 2, e]) + base
        for i, j in enumerate(pending[1:], 1):
            num[i, e] = power[b, j, e] * scaled(b)
            beside = cross[b, j, e] if j < pending[0] else cross[b, j + 2, e]
            den[i, e] = own[b, j, e] + jnp.where(lower() == (j < pending[0]), beside, 0.0) + base

    relayed = n >= 8
    relays = (side + 2, side - 3)
    side_of = (side, side - 1)

    def edge_copy(src, dst, to, send, recv):
        return pltpu.make_async_remote_copy(
            src_ref=src, dst_ref=dst, send_sem=send, recv_sem=recv,
            device_id={"shard": to}, device_id_type=MESH,
        )

    def send_edges(b):
        for way in range(2):
            cut = slice(0, EDGE) if way == 0 else slice(GB - EDGE, GB)
            for e in range(RADIX):
                x = power[b, (tiles - 1) * way, e].T[cut]
                for i in range(part // GB):
                    start = (e * (part // GB) + i) * EDGE
                    edge[b, way, start:start + EDGE] = x[:, i * GB:(i + 1) * GB]
            border = side_of[way]
            outside = me == (n - 1) * way
            if b == 0 and relayed:
                turn = me == border

                @pl.when(turn)
                def _():
                    edge_copy(edge.at[b, way], relay, relays[way], edge_send.at[way], relay_sem.at[0]).start()

                outside |= turn

            @pl.when(jnp.logical_not(outside))
            def _():
                to = lax.rem(me + (1 if way else n - 1), n)
                edge_copy(edge.at[b, way], halo.at[b, way], to, edge_send.at[way], edge_recv.at[way]).start()

    def relay_copy(way):
        to = side_of[1 - way]
        return edge_copy(relay, halo.at[0, way], to, relay_sem.at[1], edge_recv.at[way])

    def pass_edges():
        for way in range(2 if relayed else 0):
            @pl.when(me == relays[way])
            def _():
                pltpu.make_async_copy(relay, relay, relay_sem.at[0]).wait()
                relay_copy(way).start()

    def end_edges():
        for way in range(2 if relayed else 0):
            @pl.when(me == relays[way])
            def _():
                pltpu.make_async_copy(relay, relay, relay_sem.at[1]).wait()

    def take_edges():
        for way in range(2):
            @pl.when(me != (n - 1) * way)
            def _():
                gone, come = edge.at[:, way], halo.at[:, 1 - way]
                pltpu.make_async_copy(gone, gone, edge_send.at[way]).wait()
                pltpu.make_async_copy(come, come, edge_recv.at[1 - way]).wait()

        zeros = jnp.zeros((GB - 2 * EDGE, part), jnp.float32)

        def lines(b, side, e):
            start = [(e * (part // GB) + i) * EDGE for i in range(part // GB)]
            x = jnp.concatenate([halo[b, side, i:i + EDGE] for i in start], axis=1)
            return jnp.where(me > 0 if side else me < n - 1, x, 0.0)

        for b in range(beams):
            for e in range(RADIX):
                x = jnp.concatenate([lines(b, 0, e), zeros, lines(b, 1, e)], axis=0).T
                total = sums(x, band[b])[:, GB:]
                cross[b, 0, e] = total
                cross[b, tiles + 1, e] = total

    for b in range(beams):
        arrived = got.at[b, :, :, pl.ds(0, outer)]
        pltpu.make_async_copy(arrived, arrived, recv_sem.at[b, 0]).wait()
        for t in range(outer):
            transform(b, t)
        send_edges(b)

    pass_edges()
    if tiles > outer:
        for b in range(beams):
            send_slot(b, tiles - 1, near, True)
        for b in range(beams):
            send_slot(b, tiles - 1, across, False)

    done = [set() for _ in range(beams)]

    def ratios(b, ready):
        for j in range(tiles):
            if b == beams - 1 and j in pending:
                continue
            if j not in done[b] and {j - 1, j, j + 1} & set(range(tiles)) <= ready:
                for e in range(RADIX):
                    ratio(b, j, e)
                done[b].add(j)

    for t in range(outer, tiles):
        ready = set(place[:t + 1])
        for b in range(beams):
            final = t == tiles - 1 and b == beams - 1
            if final:
                if t == outer:
                    take_edges()
                    for i in range(beams - 1):
                        ratios(i, ready)
                for e in range(RADIX):
                    prepare(b, e)
                sieve[...] = band[b]
                factor[...] = jnp.full(factor.shape, scaled(b))
            arrived = got.at[b, :, :, t]
            pltpu.make_async_copy(arrived, arrived, recv_sem.at[b, t - outer + 1]).wait()
            if final:
                for e, (high, low) in enumerate(branches(b, t)):
                    tail[e, 0] = high
                    tail[e, 1] = low
                continue
            transform(b, t)
            if t == tiles - 1 and t > outer:
                ratios(b, ready)
        if t == tiles - 2:
            take_edges()
            for b in range(beams):
                ratios(b, ready)
    if tiles == outer:
        take_edges()
        for b in range(beams):
            ratios(b, set(place))

    end_edges()
    whole = sent.at[:, :, :, pl.ds(0, (n - 1) * tiles)]
    pltpu.make_async_copy(whole, whole, send_sem).wait()


def write_kernel(ratio, num, den, tail, table, sieve, factor, out, late, pw, sem):
    beams, tiles = ratio.shape[:2]
    pending = waiting(tiles)
    part = num.shape[2]

    def put(b, j):
        i = pending.index(j) if b == beams - 1 and j in pending else None
        src = ratio.at[b, j] if i is None else late.at[i]
        return pltpu.make_async_copy(src, out.at[0, b, :, pl.ds(j * GB, GB)], sem)

    for b in range(beams):
        for j in range(tiles):
            if b < beams - 1 or j not in pending:
                put(b, j).start()
    lower = lax.broadcasted_iota(jnp.int32, (part, GB), 1) < GB // 2
    if pending:
        for e in range(RADIX):
            pw[e] = intensity(table.at[e], tail[e, 0], tail[e, 1])

        for e in range(RADIX):
            p = pw[e]
            total = sums(p, sieve[...])
            for i, j in enumerate(pending):
                if i:
                    add = jnp.where(lower == (j > pending[0]), total[:, GB:], 0.0)
                else:
                    add = total[:, :GB]
                top = num[i, e] if i else p * factor[0:1]
                late.at[i][pl.ds(e, part, stride=RADIX), :] = top / (den[i, e] + add)
    for j in pending:
        put(beams - 1, j).start()
    pltpu.make_async_copy(ratio, ratio, sem).wait()


def solution(mesh):
    n = mesh.shape["shard"]

    def step(echoes, waveform, doppler_taper, cfar_guard, cfar_train, noise_floor):
        beams, local, gates = echoes.shape[2:]
        pulses = local * n
        ga = gates // GB
        tiles = ga // n
        groups = local // ROWS
        part = pulses // RADIX
        consts = tables(gates, pulses, n)
        chain, twiddle, _ = consts
        vmem = pl.BlockSpec(memory_space=pltpu.VMEM)
        hbm = pl.BlockSpec(memory_space=pltpu.HBM)
        f32, bf16, i32 = jnp.float32, jnp.bfloat16, jnp.int32
        dma = pltpu.SemaphoreType.DMA
        late = max(1, len(waiting(tiles)))
        held = [
            pltpu.VMEM(*x)
            for x in (
                ((beams, tiles, pulses, GB), f32), ((late, RADIX, part, GB), f32),
                ((late, RADIX, part, GB), f32), ((RADIX, 2, part, 2 * GB), bf16),
                ((RADIX, 2, 2 * part, part), bf16), ((2 * GB, 2 * GB), bf16), ((8, GB), f32),
            )
        ]
        room = 65456 * 1024 - sum(x.dtype.itemsize * math.prod(x.shape) for x in held)
        results = pl.pallas_call(
            functools.partial(kernel, n, beams, pulses, gates),
            out_shape=tuple(held),
            in_specs=[hbm] * 9,
            out_specs=(vmem,) * len(held),
            scratch_shapes=[
                pltpu.VMEM((beams, 2, local, gates), f32),
                pltpu.VMEM((2, ga * ROWS, GB), f32),
                pltpu.VMEM((ga, GB), f32),
                pltpu.VMEM((2, ga, GB), f32),
                pltpu.VMEM((beams, 2, groups, ga, ROWS, GB), f32),
                pltpu.VMEM((beams, 2, pulses // ROWS, tiles, ROWS, GB), f32),
                pltpu.VMEM((RADIX, 2, part, 2 * GB), bf16),
                pltpu.VMEM((beams, tiles, RADIX, part, GB), f32),
                pltpu.VMEM((beams, tiles, RADIX, part, GB), f32),
                pltpu.VMEM((beams, tiles + 2, RADIX, part, GB), f32),
                pltpu.VMEM((beams, 2, pulses // GB * EDGE, GB), f32),
                pltpu.VMEM((beams, 2, pulses // GB * EDGE, GB), f32),
                pltpu.VMEM((pulses // GB * EDGE, GB), f32),
                pltpu.VMEM((beams, 2 * GB, 2 * GB), bf16),
                pltpu.VMEM((2, gates), f32),
                pltpu.SMEM((pulses,), f32),
                pltpu.SMEM((beams,), i32),
                pltpu.SMEM((beams,), i32),
                pltpu.SMEM((beams,), f32),
                pltpu.VMEM(chain.shape, bf16),
                pltpu.VMEM(twiddle.shape, f32),
                dma((beams + 1,)),
                dma((4,)),
                dma,
                dma((beams, tiles - min(2, tiles) + 1)),
                dma((2,)),
                dma((2,)),
                dma((2,)),
            ],
            compiler_params=pltpu.CompilerParams(
                collective_id=0, has_side_effects=True, vmem_limit_bytes=room
            ),
        )(
            echoes, waveform, doppler_taper, cfar_guard, cfar_train, noise_floor,
            *(jnp.asarray(c) for c in consts),
        )
        return pl.pallas_call(
            write_kernel,
            out_shape=jax.ShapeDtypeStruct((1, beams, pulses, tiles * GB), f32),
            in_specs=[vmem] * len(held),
            out_specs=hbm,
            scratch_shapes=[pltpu.VMEM((late, pulses, GB), f32), pltpu.VMEM((RADIX, part, GB), f32), dma],
            compiler_params=pltpu.CompilerParams(vmem_limit_bytes=4096 * 1024),
        )(*results)

    in_specs = (
        P(None, None, "groups", "shard", None),
        P(),
        P(),
        P("groups"),
        P("groups"),
        P("groups"),
    )
    return jax.shard_map(
        step, mesh=mesh, in_specs=in_specs, out_specs=P(None, "groups", None, "shard"), check_vma=False
    )
```

```python
import functools
import math

import jax
import jax.numpy as jnp
import numpy as np
from jax import lax
from jax.experimental import pallas as pl
from jax.experimental.pallas import tpu as pltpu
from jax.sharding import PartitionSpec as P

GB = 128
ROWS = 8
EDGE = 20
RADIX = 4
MESH = pl.DeviceIdType.MESH


def split(table):
    table = np.asarray(table, np.float32)
    high = table.astype(jnp.bfloat16)
    low = (table - high.astype(np.float32)).astype(jnp.bfloat16)
    return high, low


def dft(length, size=None):
    size = size or length
    i = np.arange(size)[:, None] * np.arange(length)[None, :] % length
    angles = 2.0 * np.pi / length * i
    return np.cos(angles), np.sin(angles)


def slots(tiles):
    return [0, tiles - 1, *range(tiles - 2, 0, -1)][:tiles]


def waiting(tiles):
    if tiles <= 2:
        return []
    j = slots(tiles)[-1]
    return [j, j - 1, j + 1]


def tables(gates, pulses, n):
    ga = gates // GB
    tiles = ga // n
    rows = (np.arange(0, ga, tiles)[:, None] + np.array(slots(tiles))[None, :]).reshape(-1)
    ca, sa = dft(ga)
    cb, sb = dft(GB)

    def left(matrix):
        high, low = split(matrix)
        return np.block([[high, high], [low, np.zeros_like(low)]])

    first = left(np.block([[ca, sa], [-sa, ca]]))
    last = left(np.block([[ca[rows], -sa[rows]], [sa[rows], ca[rows]]]))
    per = GB // ga
    c = np.arange(GB).reshape(GB // per, per).T.reshape(-1)
    cb, sb = cb[:, c], sb[:, c]
    second = np.stack(split(np.block([[cb, -sb], [sb, cb]])))
    third = np.stack(split(np.block([[cb.T, sb.T], [-sb.T, cb.T]])))
    i = np.arange(ga)[:, None] * np.arange(GB)[None, :] % gates
    twiddle = np.stack([np.cos(2 * np.pi / gates * i), np.sin(2 * np.pi / gates * i)])
    part = pulses // RADIX
    cp, sp = dft(pulses)
    doppler = [
        np.stack(split(np.concatenate([cp[e::RADIX, :part], sp[e::RADIX, :part]], axis=0)))
        for e in range(RADIX)
    ]
    return np.stack([first, *second, *third, last]), twiddle.astype(np.float32), np.stack(doppler)


def parts(x):
    high = x.astype(jnp.bfloat16)
    low = (x - high.astype(jnp.float32)).astype(jnp.bfloat16)
    return high, low


def dot(a, b):
    return jnp.dot(a, b, preferred_element_type=jnp.float32)


def rotated(x):
    if len(x) == 2:
        return [[p + q for p, q in zip(*x)], [p - q for p, q in zip(*x)]]
    (ar, ai), (br, bi), (cr, ci), (dr, di) = x
    sr, si, tr, ti = ar + cr, ai + ci, ar - cr, ai - ci
    ur, ui, vr, vi = br + dr, bi + di, br - dr, bi - di
    return [(sr + ur, si + ui), (tr + vi, ti - vr), (sr - ur, si - ui), (tr - vi, ti + vr)]


def branches(re, im):
    x = [y.reshape(RADIX, -1, GB) for y in (re, im)]
    return [parts(jnp.concatenate(y, axis=1)) for y in rotated([(x[0][i], x[1][i]) for i in range(RADIX)])]


def stacked(high, low, axis):
    return jnp.concatenate([high, high, low] if axis else [high, low, high], axis=axis)


def intensity(table, high, low):
    spec = dot(stacked(table[0], table[1], 1), stacked(high, low, 0))
    part = spec.shape[0] // 2
    re = spec[:part, :GB] + spec[part:, GB:]
    im = spec[:part, GB:] - spec[part:, :GB]
    return re * re + im * im


def sums(x, band):
    return dot(jnp.concatenate(parts(x), axis=1), band)


def kernel(
    n, beams, pulses, gates,
    echoes, waveform_hbm, taper_hbm, guard_hbm, train_hbm, floor_hbm,
    chain_hbm, twiddle_hbm, doppler_hbm,
    out, num, den, tail, table, sieve, factor,
    xin, xs, wave, filt, sent, got, rhs, power, own, cross, edge, halo, relay, band,
    waveform, taper, guard, train, floor, chain, twiddle,
    in_sem, small_sem, send_sem, recv_sem, edge_send, edge_recv, relay_sem,
):
    me = lax.axis_index("shard")
    ga = gates // GB
    tiles = ga // n
    groups = pulses // n // ROWS
    part = pulses // RADIX
    place = slots(tiles)
    outer = min(2, tiles)
    side = n // 2
    mine = lax.rem(me, side)
    far, here = side - (me - mine), me - mine
    across = [far + k for k in range(side)]
    near = [here + lax.rem(mine + k, side) for k in range(1, side)]
    order = across[:1] + [to for pair in zip(near, across[1:]) for to in pair]

    barrier = pltpu.get_barrier_semaphore()
    for to in order:
        pl.semaphore_signal(barrier, inc=1, device_id={"shard": to}, device_id_type=MESH)

    def load(b, start, size, sem):
        return pltpu.make_async_copy(
            echoes.at[0, :, b, pl.ds(start, size), :], xin.at[b, :, pl.ds(start, size)], in_sem.at[sem]
        )

    local = groups * ROWS
    loads = [load(0, 0, ROWS, beams)]
    loads += [load(0, ROWS, local - ROWS, 0)] if groups > 1 else []
    loads += [load(b, 0, local, b) for b in range(1, beams)]
    small = [
        pltpu.make_async_copy(src, dst, small_sem.at[i])
        for i, (src, dst) in enumerate(
            ((waveform_hbm, waveform), (chain_hbm, chain), (twiddle_hbm, twiddle), (taper_hbm, taper))
        )
    ]
    later = [
        pltpu.make_async_copy(src, dst, small_sem.at[i])
        for i, (src, dst) in enumerate(
            ((doppler_hbm, table), (guard_hbm, guard), (train_hbm, train), (floor_hbm, floor))
        )
    ]
    small[0].start()
    loads[0].start()
    for copy in small[1:]:
        copy.start()

    per = GB // ga
    scale = 1.0 / (gates * math.sqrt(pulses))
    small[0].wait()
    for c in range(2):
        for m in range(ga):
            wave[m:m + 1, :] = waveform[c:c + 1, m * GB:(m + 1) * GB]
        lines = wave[...] * scale
        turned = [lines] + [pltpu.roll(lines, GB - h * ga, axis=1) for h in range(1, per)]
        filt[c] = jnp.concatenate(turned, axis=0).T[:ga]
    def stage(i):
        return jnp.concatenate([chain[i], chain[i], chain[i + 1]], axis=0)

    def compress(b, pg):
        row = pg * ROWS if isinstance(pg, int) else pl.multiple_of(pg * ROWS, ROWS)
        for c in range(2):
            for i in range(ga):
                xs[c, i * ROWS:(i + 1) * ROWS, :] = xin[b, c, pl.ds(row, ROWS), i * GB:(i + 1) * GB]
        tc, ts = twiddle[0], twiddle[1]
        lhs = []
        for p in range(0, ROWS, 2):
            x = jnp.concatenate(
                [
                    jnp.concatenate([xs[c, pl.ds(p + e, ga, stride=ROWS), :] for c in range(2)], axis=0)
                    for e in range(2)
                ],
                axis=1,
            )
            y = dot(chain[0], jnp.concatenate(parts(x), axis=0))
            y = y[:2 * ga] + y[2 * ga:]
            for e in range(2):
                yr, yi = y[:ga, e * GB:(e + 1) * GB], y[ga:, e * GB:(e + 1) * GB]
                z = jnp.concatenate([yr * tc + yi * ts, yi * tc - yr * ts], axis=1)
                high, low = parts(z)
                lhs.append(jnp.concatenate([high, low, high], axis=1))
        x = dot(jnp.concatenate(lhs, axis=0), stage(1))
        lhs = []
        fr, fi = filt[0], filt[1]
        for p in range(ROWS):
            weight = taper[(me * groups + pg) * ROWS + p]
            hr, hi = fr * weight, fi * weight
            xr, xi = x[p * ga:(p + 1) * ga, :GB], x[p * ga:(p + 1) * ga, GB:]
            z = jnp.concatenate([xr * hr + xi * hi, xi * hr - xr * hi], axis=1)
            high, low = parts(z)
            lhs.append(jnp.concatenate([high, low, high], axis=1))
        x = dot(jnp.concatenate(lhs, axis=0), stage(3))
        for p in range(0, ROWS, 2):
            pair = []
            for e in range(2):
                r = (p + e) * ga
                xr, xi = x[r:r + ga, :GB], x[r:r + ga, GB:]
                pair.append(jnp.concatenate([xr * tc - xi * ts, xi * tc + xr * ts], axis=0))
            y = dot(chain[5], jnp.concatenate(parts(jnp.concatenate(pair, axis=1)), axis=0))
            y = y[:2 * ga] + y[2 * ga:]
            for e in range(2):
                for c in range(2):
                    sent.at[b, c, pg].reshape(ga * ROWS, GB)[pl.ds(p + e, ga, stride=ROWS), :] = y[
                        c * ga:(c + 1) * ga, e * GB:(e + 1) * GB
                    ]

    def send(src, dst, sem, peers, keep):
        for to in peers:
            pltpu.make_async_remote_copy(
                src_ref=src(to),
                dst_ref=dst,
                send_sem=send_sem,
                recv_sem=sem,
                device_id={"shard": to},
                device_id_type=MESH,
            ).start()
        if keep:
            pltpu.make_async_copy(src(me), dst, sem).start()

    def send_groups(b, pg, count):
        send(
            lambda to: sent.at[b, :, pl.ds(pg, count), pl.ds(to * tiles, outer)],
            got.at[b, :, pl.ds(me * groups + pg, count), pl.ds(0, outer)],
            recv_sem.at[b, 0], order, True,
        )

    def send_slot(b, t, peers, keep):
        send(
            lambda to: sent.at[b, :, :, to * tiles + t],
            tail.at[:, pl.ds(me * groups, groups)] if (b, t) == (beams - 1, tiles - 1) else got.at[b, :, pl.ds(me * groups, groups), t],
            recv_sem.at[b, t - outer + 1], peers, keep,
        )

    for copy in small[1:]:
        copy.wait()
    loads[0].wait()
    for copy in loads[1:2]:
        copy.start()
    compress(0, 0)
    pl.semaphore_wait(barrier, n - 1)
    send_groups(0, 0, 1)
    for copy in loads[2:] + later:
        copy.start()
    for b in range(beams):
        begin = 1 if b == 0 else 0
        if begin < groups:
            loads[b + 1 if groups > 1 else b].wait()

        @pl.loop(begin, groups)
        def _(pg):
            compress(b, pg)

            @pl.when(lax.rem(pg - begin, 2) == 1)
            def _():
                send_groups(b, pg - 1, 2)

            if (groups - begin) % 2:
                @pl.when(pg == groups - 1)
                def _():
                    send_groups(b, pg, 1)

    for t in range(outer, tiles - 1):
        for b in range(beams):
            send_slot(b, t, order, True)

    for copy in later:
        copy.wait()

    m = lax.broadcasted_iota(jnp.int32, (GB, 2 * GB), 0)
    k = lax.broadcasted_iota(jnp.int32, (GB, 2 * GB), 1)
    apart = jnp.where(k < GB, jnp.abs(m - k), jnp.where(k < GB + GB // 2, k - m, m + 2 * GB - k))
    for b in range(beams):
        inside = (apart > guard[b]) & (apart <= guard[b] + train[b])
        lines = jnp.where(inside, 1.0, 0.0).astype(jnp.bfloat16)
        band[b, :GB] = lines
        band[b, GB:] = lines

    pending = waiting(tiles)

    def transform(b, t):
        j = place[t]
        for e, (high, low) in enumerate(branches(got[b, 0, :, t], got[b, 1, :, t])):
            rhs[e, 0] = high
            rhs[e, 1] = low
        for e in range(RADIX):
            p = intensity(table.at[e], rhs[e, 0], rhs[e, 1])
            power[b, j, e] = p
            total = sums(p, band[b])
            own[b, j, e] = total[:, :GB]
            cross[b, j + 1, e] = total[:, GB:]

    def scaled(b):
        return 2.0 * train[b].astype(jnp.float32)

    def lower():
        return lax.broadcasted_iota(jnp.int32, (part, GB), 1) < GB // 2

    def ratio(b, j, e):
        total = own[b, j, e] + jnp.where(lower(), cross[b, j, e], cross[b, j + 2, e])
        out.at[b, j][pl.ds(e, part, stride=RADIX), :] = (
            power[b, j, e] * scaled(b) / (floor[b] * scaled(b) + total)
        )

    def prepare(b, e):
        base = floor[b] * scaled(b)
        den[0, e] = jnp.where(lower(), cross[b, pending[0], e], cross[b, pending[0] + 2, e]) + base
        for i, j in enumerate(pending[1:], 1):
            num[i, e] = power[b, j, e] * scaled(b)
            beside = cross[b, j, e] if j < pending[0] else cross[b, j + 2, e]
            den[i, e] = own[b, j, e] + jnp.where(lower() == (j < pending[0]), beside, 0.0) + base

    relayed = n >= 8
    relays = (side + 2, side - 3)
    side_of = (side, side - 1)

    def edge_copy(src, dst, to, send, recv):
        return pltpu.make_async_remote_copy(
            src_ref=src, dst_ref=dst, send_sem=send, recv_sem=recv,
            device_id={"shard": to}, device_id_type=MESH,
        )

    def send_edges(b):
        for way in range(2):
            cut = slice(0, EDGE) if way == 0 else slice(GB - EDGE, GB)
            for e in range(RADIX):
                x = power[b, (tiles - 1) * way, e].T[cut]
                for i in range(part // GB):
                    start = (e * (part // GB) + i) * EDGE
                    edge[b, way, start:start + EDGE] = x[:, i * GB:(i + 1) * GB]
            border = side_of[way]
            outside = me == (n - 1) * way
            if b == 0 and relayed:
                turn = me == border

                @pl.when(turn)
                def _():
                    edge_copy(edge.at[b, way], relay, relays[way], edge_send.at[way], relay_sem.at[0]).start()

                outside |= turn

            @pl.when(jnp.logical_not(outside))
            def _():
                to = lax.rem(me + (1 if way else n - 1), n)
                edge_copy(edge.at[b, way], halo.at[b, way], to, edge_send.at[way], edge_recv.at[way]).start()

    def relay_copy(way):
        to = side_of[1 - way]
        return edge_copy(relay, halo.at[0, way], to, relay_sem.at[1], edge_recv.at[way])

    def pass_edges():
        for way in range(2 if relayed else 0):
            @pl.when(me == relays[way])
            def _():
                pltpu.make_async_copy(relay, relay, relay_sem.at[0]).wait()
                relay_copy(way).start()

    def end_edges():
        for way in range(2 if relayed else 0):
            @pl.when(me == relays[way])
            def _():
                pltpu.make_async_copy(relay, relay, relay_sem.at[1]).wait()

    def take_edges():
        for way in range(2):
            @pl.when(me != (n - 1) * way)
            def _():
                gone, come = edge.at[:, way], halo.at[:, 1 - way]
                pltpu.make_async_copy(gone, gone, edge_send.at[way]).wait()
                pltpu.make_async_copy(come, come, edge_recv.at[1 - way]).wait()

        zeros = jnp.zeros((GB - 2 * EDGE, part), jnp.float32)

        def lines(b, side, e):
            start = [(e * (part // GB) + i) * EDGE for i in range(part // GB)]
            x = jnp.concatenate([halo[b, side, i:i + EDGE] for i in start], axis=1)
            return jnp.where(me > 0 if side else me < n - 1, x, 0.0)

        for b in range(beams):
            for e in range(RADIX):
                x = jnp.concatenate([lines(b, 0, e), zeros, lines(b, 1, e)], axis=0).T
                total = sums(x, band[b])[:, GB:]
                cross[b, 0, e] = total
                cross[b, tiles + 1, e] = total

    for b in range(beams):
        arrived = got.at[b, :, :, pl.ds(0, outer)]
        pltpu.make_async_copy(arrived, arrived, recv_sem.at[b, 0]).wait()
        for t in range(outer):
            transform(b, t)
        send_edges(b)

    pass_edges()
    if tiles > outer:
        for b in range(beams):
            send_slot(b, tiles - 1, near, True)
        for b in range(beams):
            send_slot(b, tiles - 1, across, False)

    done = [set() for _ in range(beams)]

    def ratios(b, ready):
        for j in range(tiles):
            if b == beams - 1 and j in pending:
                continue
            if j not in done[b] and {j - 1, j, j + 1} & set(range(tiles)) <= ready:
                for e in range(RADIX):
                    ratio(b, j, e)
                done[b].add(j)

    for t in range(outer, tiles):
        ready = set(place[:t + 1])
        for b in range(beams):
            final = t == tiles - 1 and b == beams - 1
            if final:
                if t == outer:
                    take_edges()
                    for i in range(beams - 1):
                        ratios(i, ready)
                for e in range(RADIX):
                    prepare(b, e)
                sieve[...] = band[b]
                factor[...] = jnp.full(factor.shape, scaled(b))
            arrived = tail if final else got.at[b, :, :, t]
            pltpu.make_async_copy(arrived, arrived, recv_sem.at[b, t - outer + 1]).wait()
            if final:
                continue
            transform(b, t)
            if t == tiles - 1 and t > outer:
                ratios(b, ready)
        if t == tiles - 2:
            take_edges()
            for b in range(beams):
                ratios(b, ready)
    if tiles == outer:
        take_edges()
        for b in range(beams):
            ratios(b, set(place))

    end_edges()
    whole = sent.at[:, :, :, pl.ds(0, (n - 1) * tiles)]
    pltpu.make_async_copy(whole, whole, send_sem).wait()


def write_kernel(ratio, num, den, tail, table, sieve, factor, out, late, pw, split_in, sem):
    beams, tiles = ratio.shape[:2]
    pending = waiting(tiles)
    part = num.shape[2]

    def put(b, j):
        i = pending.index(j) if b == beams - 1 and j in pending else None
        src = ratio.at[b, j] if i is None else late.at[i]
        return pltpu.make_async_copy(src, out.at[0, b, :, pl.ds(j * GB, GB)], sem)

    for b in range(beams):
        for j in range(tiles):
            if b < beams - 1 or j not in pending:
                put(b, j).start()
    lower = lax.broadcasted_iota(jnp.int32, (part, GB), 1) < GB // 2
    if pending:
        for e, (high, low) in enumerate(branches(tail[0], tail[1])):
            split_in[e, 0] = high
            split_in[e, 1] = low
        for e in range(RADIX):
            pw[e] = intensity(table.at[e], split_in[e, 0], split_in[e, 1])

        for e in range(RADIX):
            p = pw[e]
            total = sums(p, sieve[...])
            for i, j in enumerate(pending):
                if i:
                    add = jnp.where(lower == (j > pending[0]), total[:, GB:], 0.0)
                else:
                    add = total[:, :GB]
                top = num[i, e] if i else p * factor[0:1]
                late.at[i][pl.ds(e, part, stride=RADIX), :] = top / (den[i, e] + add)
    for j in pending:
        put(beams - 1, j).start()
    pltpu.make_async_copy(ratio, ratio, sem).wait()


def solution(mesh):
    n = mesh.shape["shard"]

    def step(echoes, waveform, doppler_taper, cfar_guard, cfar_train, noise_floor):
        beams, local, gates = echoes.shape[2:]
        pulses = local * n
        ga = gates // GB
        tiles = ga // n
        groups = local // ROWS
        part = pulses // RADIX
        consts = tables(gates, pulses, n)
        chain, twiddle, _ = consts
        vmem = pl.BlockSpec(memory_space=pltpu.VMEM)
        hbm = pl.BlockSpec(memory_space=pltpu.HBM)
        f32, bf16, i32 = jnp.float32, jnp.bfloat16, jnp.int32
        dma = pltpu.SemaphoreType.DMA
        late = max(1, len(waiting(tiles)))
        held = [
            pltpu.VMEM(*x)
            for x in (
                ((beams, tiles, pulses, GB), f32), ((late, RADIX, part, GB), f32),
                ((late, RADIX, part, GB), f32), ((2, pulses // ROWS, ROWS, GB), f32),
                ((RADIX, 2, 2 * part, part), bf16), ((2 * GB, 2 * GB), bf16), ((8, GB), f32),
            )
        ]
        room = 65456 * 1024 - sum(x.dtype.itemsize * math.prod(x.shape) for x in held)
        results = pl.pallas_call(
            functools.partial(kernel, n, beams, pulses, gates),
            out_shape=tuple(held),
            in_specs=[hbm] * 9,
            out_specs=(vmem,) * len(held),
            scratch_shapes=[
                pltpu.VMEM((beams, 2, local, gates), f32),
                pltpu.VMEM((2, ga * ROWS, GB), f32),
                pltpu.VMEM((ga, GB), f32),
                pltpu.VMEM((2, ga, GB), f32),
                pltpu.VMEM((beams, 2, groups, ga, ROWS, GB), f32),
                pltpu.VMEM((beams, 2, pulses // ROWS, tiles, ROWS, GB), f32),
                pltpu.VMEM((RADIX, 2, part, 2 * GB), bf16),
                pltpu.VMEM((beams, tiles, RADIX, part, GB), f32),
                pltpu.VMEM((beams, tiles, RADIX, part, GB), f32),
                pltpu.VMEM((beams, tiles + 2, RADIX, part, GB), f32),
                pltpu.VMEM((beams, 2, pulses // GB * EDGE, GB), f32),
                pltpu.VMEM((beams, 2, pulses // GB * EDGE, GB), f32),
                pltpu.VMEM((pulses // GB * EDGE, GB), f32),
                pltpu.VMEM((beams, 2 * GB, 2 * GB), bf16),
                pltpu.VMEM((2, gates), f32),
                pltpu.SMEM((pulses,), f32),
                pltpu.SMEM((beams,), i32),
                pltpu.SMEM((beams,), i32),
                pltpu.SMEM((beams,), f32),
                pltpu.VMEM(chain.shape, bf16),
                pltpu.VMEM(twiddle.shape, f32),
                dma((beams + 1,)),
                dma((4,)),
                dma,
                dma((beams, tiles - min(2, tiles) + 1)),
                dma((2,)),
                dma((2,)),
                dma((2,)),
            ],
            compiler_params=pltpu.CompilerParams(
                collective_id=0, has_side_effects=True, vmem_limit_bytes=room
            ),
        )(
            echoes, waveform, doppler_taper, cfar_guard, cfar_train, noise_floor,
            *(jnp.asarray(c) for c in consts),
        )
        return pl.pallas_call(
            write_kernel,
            out_shape=jax.ShapeDtypeStruct((1, beams, pulses, tiles * GB), f32),
            in_specs=[vmem] * len(held),
            out_specs=hbm,
            scratch_shapes=[pltpu.VMEM((late, pulses, GB), f32), pltpu.VMEM((RADIX, part, GB), f32), pltpu.VMEM((RADIX, 2, part, 2 * GB), bf16), dma],
            compiler_params=pltpu.CompilerParams(vmem_limit_bytes=4096 * 1024),
        )(*results)

    in_specs = (
        P(None, None, "groups", "shard", None),
        P(),
        P(),
        P("groups"),
        P("groups"),
        P("groups"),
    )
    return jax.shard_map(
        step, mesh=mesh, in_specs=in_specs, out_specs=P(None, "groups", None, "shard"), check_vma=False
    )
```
